256 devices in a mesh: dp: 64 (over x_lo, y, z), mp: 2 (over core), fsdp: 2 (over x_hi).
Axes of the slice: x: 4 (x_hi: 2, x_lo: 2; x = x_hi * 2 + x_lo), y: 4, z: 8, core: 2. Of those that a mesh axis runs over, the one named last changes fastest.
Arguments:
- features: bfloat16 [5, 1024, 4096], P(None, ('dp', 'fsdp')), may hold values from -24 to 24
- memory_bank: bfloat16 [4096, 32, 1024], P(('dp', 'fsdp')), may hold values from -1 to 1
- memory_fill: int32 [4096], P(('dp', 'fsdp')), may hold values from 0 to 32
- left_keys: bfloat16 [4096, 64, 1024], P(('dp', 'fsdp'), None, 'mp'), may hold values from -400 to 400
- left_values: bfloat16 [4096, 64, 1024], P(('dp', 'fsdp'), None, 'mp'), may hold values from -6 to 6
- left_length: int32 [4096], P(('dp', 'fsdp')), may hold values from 0 to 64
- w_query: bfloat16 [1024, 1024], P('fsdp', 'mp'), may hold values from -0.1875 to 0.1875
- w_key: bfloat16 [1024, 1024], P('fsdp', 'mp'), may hold values from -0.1875 to 0.1875
- w_value: bfloat16 [1024, 1024], P('fsdp', 'mp'), may hold values from -0.1875 to 0.1875
- w_out: bfloat16 [1024, 1024], P('mp', 'fsdp'), may hold values from -0.1875 to 0.1875
- w_up: bfloat16 [1024, 4096], P('fsdp', 'mp'), may hold values from -0.1875 to 0.1875
- w_down: bfloat16 [4096, 1024], P('mp', 'fsdp'), may hold values from -0.09375 to 0.09375
- out_gain: float32 [1024], replicated, may hold values from 0.1 to 1.9
Outputs:
- layer_out: bfloat16 [4096, 5, 1024], P(('dp', 'fsdp'))
- memory_next: bfloat16 [4096, 1024], P(('dp', 'fsdp'))
- center_keys: bfloat16 [4096, 4, 1024], P(('dp', 'fsdp'), None, 'mp')
- center_values: bfloat16 [4096, 4, 1024], P(('dp', 'fsdp'), None, 'mp')
The draws below stay inside these ranges and needn't reach their ends.
All inputs are finite; a program needn't handle non-finite values.
Results may differ from the reference program's by a relative error of at most 0.0095.
Values may be sent and summed in bfloat16 or wider, within the bound.
A program may use at most 128 MiB of HBM per device.

```python
import jax
import jax.numpy as jnp
from jax import lax

D = 1024
H = 16
HD = 64
FF = 4096
MEM = 32
LEFT = 64
GROUP = 4
FRAMES = 5
STR_DEV = 32
STREAMS = 4096


def draw_left_keys(key, part):
    base = jnp.clip(jax.random.normal(jax.random.fold_in(key, 11), (STREAMS, LEFT, D), jnp.float32), -6.0, 6.0)
    return base.astype(jnp.bfloat16)


def set_ends(entries, key, least, top_value):
    place = [jax.random.randint(jax.random.fold_in(key, axis), (), 0, length) for axis, length in enumerate(entries.shape)]
    main_axis = entries.shape.index(max(entries.shape))
    beside = place[:main_axis] + [(place[main_axis] + 1) % entries.shape[main_axis]] + place[main_axis + 1:]
    return entries.at[tuple(place)].set(least).at[tuple(beside)].set(top_value)


def raised(values, key, source, target, parts, factor):
    def block_of(dim):
        return (jnp.arange(values.shape[dim]) // (values.shape[dim] // parts)).reshape((-1,) + (1,) * (values.ndim - 1 - dim))

    one_side = jax.random.permutation(key, parts)[block_of(target)]
    second = (block_of(target) + parts // 2) % parts
    return jnp.where((block_of(source) == one_side) | (block_of(source) == second), factor * values, values)


def levels(own_key, extent, pieces, smallest, top_value):
    level = 1.0
    for position, shards_of in pieces:
        heights = jax.random.uniform(jax.random.fold_in(jax.random.fold_in(own_key, 6), position), (shards_of,), jnp.float32, smallest / len(pieces), top_value / len(pieces))
        level = level * jnp.repeat(jnp.exp(heights), extent[position] // shards_of).reshape((-1,) + (1,) * (len(extent) - 1 - position))
    return level


def normal_values(stream_key, dims, width, most, shards=(), held_as=jnp.bfloat16):
    values = jax.random.normal(stream_key, dims, jnp.float32) * width
    if len(shards) > 0:
        values = levels(stream_key, dims, shards, -0.22, 0.18) * values
    return jnp.clip(values, min=-most, max=most).astype(held_as)


def bell_draw_with(stream_key, shape, width, limit, cuts, heavy, kind=jnp.bfloat16):
    values = width * jax.random.normal(stream_key, shape, jnp.float32)
    if cuts:
        values = values * levels(stream_key, shape, cuts, -0.22, 0.18)
    return jnp.clip(raised(values, jax.random.fold_in(stream_key, 3), *heavy), -limit, limit).astype(kind)


def setup_inputs(seed: int = 0) -> dict:
    streams_of = jax.random.split(jax.random.key(seed), 14)
    features = bell_draw_with(streams_of[0], (FRAMES, D, STREAMS), 1.0, 24.0, ((1, 128),), (1, 2, 128, 5.5))
    memory_bank = jnp.clip(jax.random.uniform(streams_of[1], (STREAMS, MEM, D), jnp.float32, -1.0, 1.0) * levels(streams_of[1], (STREAMS, MEM, D), ((0, 128),), -0.4, 0.0), -1.0, 1.0).astype(jnp.bfloat16)
    memory_fill = set_ends(jax.random.randint(streams_of[2], (STREAMS,), 0, MEM + 1), jax.random.fold_in(streams_of[2], 1), 0, MEM).astype(jnp.int32)
    left_keys = draw_left_keys(jax.random.fold_in(streams_of[13], 71), 0)
    left_values = normal_values(streams_of[4], (STREAMS, LEFT, D), 1.0, 6.0, ((0, 128), (2, 2)))
    left_length = set_ends(jax.random.randint(streams_of[5], (STREAMS,), 0, LEFT + 1), jax.random.fold_in(streams_of[5], 1), 0, LEFT).astype(jnp.int32)
    w_query = normal_values(streams_of[6], (D, D), D ** -0.5, 0.1875, ((0, 2), (1, 2)))
    w_key = normal_values(streams_of[7], (D, D), D ** -0.5, 0.1875, ((0, 2), (1, 2)))
    w_value = normal_values(streams_of[8], (D, D), D ** -0.5, 0.1875, ((0, 2), (1, 2)))
    w_out = normal_values(streams_of[9], (D, D), D ** -0.5, 0.1875, ((0, 2), (1, 2)))
    w_up = normal_values(streams_of[10], (D, FF), D ** -0.5, 0.1875, ((0, 2), (1, 2)))
    w_down = normal_values(streams_of[11], (FF, D), FF ** -0.5, 0.09375, ((0, 2), (1, 2)))
    out_gain = jnp.clip(1.0 + 0.18 * jax.random.normal(streams_of[12], (D,), jnp.float32), 0.1, 1.9)
    return {"features": features, "memory_bank": memory_bank, "memory_fill": memory_fill, "left_keys": left_keys, "left_values": left_values, "left_length": left_length, "w_query": w_query, "w_key": w_key, "w_value": w_value, "w_out": w_out, "w_up": w_up, "w_down": w_down, "out_gain": out_gain}


epsilon = 1e-05
masked_score = -1e+30

def normalize(values):
    values = values.astype(jnp.float32)
    average = lax.optimization_barrier(jnp.mean(values, axis=-1, keepdims=True))
    centred = values - average
    variance = lax.optimization_barrier(jnp.mean(centred * centred, axis=-1, keepdims=True))
    return centred * lax.rsqrt(variance + epsilon)

def visible_masks(fill, length, mem_slots, left_slots, query_count):
    mem_ok = jnp.arange(mem_slots, dtype=jnp.int32)[None, :] >= (mem_slots - fill)[:, None]
    not_summary = jnp.arange(query_count, dtype=jnp.int32) < query_count - 1
    mem_mask = mem_ok[:, None, None, :] & not_summary[None, None, :, None]
    left_ok = jnp.arange(left_slots, dtype=jnp.int32)[None, :] >= (left_slots - length)[:, None]
    left_mask = left_ok[:, None, None, :] & (not_summary[None, None, :, None] | True)
    return (mem_mask, left_mask)

def reference(features, memory_bank, memory_fill, left_keys, left_values, left_length, w_query, w_key, w_value, w_out, w_up, w_down, out_gain):
    streams = features.shape[2]
    inputs = jnp.transpose(features, (2, 0, 1))
    normed = normalize(inputs).astype(jnp.bfloat16)
    summary = lax.optimization_barrier(jnp.mean(normed[:, :GROUP, :].astype(jnp.float32), axis=1)).astype(jnp.bfloat16)
    query_rows = jnp.concatenate([normed, summary[:, None, :]], axis=1).reshape(-1, D)
    query_proj = jnp.dot(query_rows, w_query, preferred_element_type=jnp.float32).astype(jnp.bfloat16)
    group_rows = normed.reshape(-1, D)
    group_keys = jnp.dot(group_rows, w_key, preferred_element_type=jnp.float32).astype(jnp.bfloat16)
    group_values = jnp.dot(group_rows, w_value, preferred_element_type=jnp.float32).astype(jnp.bfloat16)
    blocks = streams // STR_DEV
    scale = HD ** (-0.5)

    def split(array):
        return array.reshape((blocks, STR_DEV) + array.shape[1:])

    def attend(operands):
        query_blk, ckey_blk, cval_blk, memory_blk, lkey_blk, lval_blk, fill_blk, length_blk = operands
        memory_rows = memory_blk.reshape(-1, D)
        mem_keys = jnp.dot(memory_rows, w_key, preferred_element_type=jnp.float32).astype(jnp.bfloat16)
        mem_values = jnp.dot(memory_rows, w_value, preferred_element_type=jnp.float32).astype(jnp.bfloat16)
        query_h = query_blk.reshape(STR_DEV, FRAMES + 1, H, HD).astype(jnp.float32)
        mkey_h = mem_keys.reshape(STR_DEV, MEM, H, HD).astype(jnp.float32)
        mval_h = mem_values.reshape(STR_DEV, MEM, H, HD).astype(jnp.float32)
        lkey_h = lkey_blk.reshape(STR_DEV, LEFT, H, HD).astype(jnp.float32)
        lval_h = lval_blk.reshape(STR_DEV, LEFT, H, HD).astype(jnp.float32)
        ckey_h = ckey_blk.reshape(STR_DEV, FRAMES, H, HD).astype(jnp.float32)
        cval_h = cval_blk.reshape(STR_DEV, FRAMES, H, HD).astype(jnp.float32)
        mem_mask, left_mask = visible_masks(fill_blk, length_blk, MEM, LEFT, FRAMES + 1)
        score_mem = jnp.einsum('sqhd,skhd->shqk', query_h, mkey_h) * scale
        score_left = jnp.einsum('sqhd,skhd->shqk', query_h, lkey_h) * scale
        score_group = jnp.einsum('sqhd,skhd->shqk', query_h, ckey_h) * scale
        score_mem = jnp.where(mem_mask, score_mem, masked_score)
        score_left = jnp.where(left_mask, score_left, masked_score)
        top = jnp.maximum(jnp.maximum(lax.optimization_barrier(jnp.max(score_mem, axis=-1, keepdims=True)), lax.optimization_barrier(jnp.max(score_left, axis=-1, keepdims=True))), lax.optimization_barrier(jnp.max(score_group, axis=-1, keepdims=True)))
        exp_mem = jnp.exp(score_mem - top)
        exp_left = jnp.exp(score_left - top)
        exp_group = jnp.exp(score_group - top)
        totals = lax.optimization_barrier(jnp.sum(exp_mem, axis=-1, keepdims=True)) + lax.optimization_barrier(jnp.sum(exp_left, axis=-1, keepdims=True)) + lax.optimization_barrier(jnp.sum(exp_group, axis=-1, keepdims=True))
        prob_mem = (exp_mem / totals).astype(jnp.bfloat16).astype(jnp.float32)
        prob_left = (exp_left / totals).astype(jnp.bfloat16).astype(jnp.float32)
        prob_group = (exp_group / totals).astype(jnp.bfloat16).astype(jnp.float32)
        attended = jnp.einsum('shqk,skhd->sqhd', prob_mem, mval_h) + jnp.einsum('shqk,skhd->sqhd', prob_left, lval_h) + jnp.einsum('shqk,skhd->sqhd', prob_group, cval_h)
        return attended.astype(jnp.bfloat16).reshape(STR_DEV, FRAMES + 1, D)
    attended = lax.map(attend, (split(query_proj.reshape(streams, (FRAMES + 1) * D)), split(group_keys.reshape(streams, FRAMES * D)), split(group_values.reshape(streams, FRAMES * D)), split(memory_bank), split(left_keys), split(left_values), split(memory_fill), split(left_length)))
    attended = attended.reshape(-1, D)
    attn_out = jnp.dot(attended, w_out, preferred_element_type=jnp.float32).reshape(streams, FRAMES + 1, D)
    memory_next = jnp.tanh(attn_out[:, FRAMES, :]).astype(jnp.bfloat16)
    hidden_state = inputs.astype(jnp.float32) + attn_out[:, :FRAMES, :]
    h_norm = normalize(hidden_state).astype(jnp.bfloat16).reshape(-1, D)
    up_proj = jax.nn.gelu(jnp.dot(h_norm, w_up, preferred_element_type=jnp.float32), approximate=True).astype(jnp.bfloat16)
    down_proj = jnp.dot(up_proj, w_down, preferred_element_type=jnp.float32)
    layer_out = (normalize(hidden_state.reshape(-1, D) + down_proj) * out_gain.astype(jnp.float32)).astype(jnp.bfloat16).reshape(streams, FRAMES, D)
    center_keys = group_keys.reshape(streams, FRAMES, D)[:, :GROUP, :]
    center_values = group_values.reshape(streams, FRAMES, D)[:, :GROUP, :]
    return (layer_out, memory_next, center_keys, center_values)
```

```python
import functools

import jax
import jax.numpy as jnp
from jax import lax
from jax.experimental import pallas as pl
from jax.experimental.pallas import tpu as pltpu
from jax.sharding import PartitionSpec as P

HD = 64
GROUP = 4
FRAMES = 5
MEM = 32
LEFT = 64
STR = 32
ROWS = 8
KEYS = 112
UNITS = 12
EPS = 1e-05
MASKED = -1e30
F32 = jnp.float32
BF16 = jnp.bfloat16


def dot(a, b):
    return jnp.dot(a, b, preferred_element_type=F32)


def normalized(x):
    mean = jnp.sum(x, axis=-1, keepdims=True) * (1.0 / x.shape[-1])
    cent = x - mean
    var = jnp.sum(cent * cent, axis=-1, keepdims=True) * (1.0 / x.shape[-1])
    return cent * lax.rsqrt(var + EPS)


def kernel(
    fill,
    length,
    feat_hbm,
    mem_hbm,
    lk_hbm,
    lv_hbm,
    wq_hbm,
    wk_hbm,
    wv_hbm,
    wo_hbm,
    wu_hbm,
    wd_hbm,
    gain,
    out,
    mem_next,
    center_k,
    center_v,
    feat,
    gath,
    blocks,
    held,
    perm,
    rows,
    xp,
    x,
    n,
    own,
    got,
    memory,
    keys,
    values,
    q,
    att,
    part,
    part_in,
    down,
    down_out,
    down_in,
    l_sem,
    g_send,
    g_recv,
    h_send,
    h_recv,
    c_send,
    c_recv,
    f_send,
    f_recv,
    e_send,
    e_recv,
):
    d = lax.axis_index("dp")
    m = lax.axis_index("mp")
    f = lax.axis_index("fsdp")
    xl = lax.div(d, 32)
    y = lax.rem(lax.div(d, 8), 4)
    z = lax.rem(d, 8)
    k = lax.div(d, 2)
    odd = lax.rem(d, 2)
    r = odd * 2 + f
    slot = r * 2 + m
    color = lax.rem(y + 2 * xl, 4)

    def dev(dd, ff, mm):
        return {"dp": dd, "fsdp": ff, "mp": mm}

    def remote(src, dst, send, recv, to):
        return pltpu.make_async_remote_copy(
            src_ref=src,
            dst_ref=dst,
            send_sem=send,
            recv_sem=recv,
            device_id=to,
            device_id_type=pl.DeviceIdType.MESH,
        )

    flipped = d + 32 * (1 - 2 * xl)
    up_d = xl * 32 + lax.rem(y + 1, 4) * 8 + z
    down_d = xl * 32 + lax.rem(y + 3, 4) * 8 + z
    cross_dev = dev(flipped, 1 - f, m)
    ring = (dev(flipped, f, m), dev(up_d, f, m), dev(down_d, f, m))
    sibling = dev(d, f, 1 - m)

    def load(i, src, dst):
        return pltpu.make_async_copy(src, dst, l_sem.at[i])

    units = [wk_hbm, wv_hbm, wq_hbm, wo_hbm]
    for j in range(4):
        units.append(wu_hbm.at[:, pl.ds(512 * j, 512)])
        units.append(wd_hbm.at[pl.ds(512 * j, 512), :])
    loads = [load(u, units[u], own.at[u]) for u in range(UNITS)]
    load_feat = load(UNITS, feat_hbm, feat)
    load_mem = load(UNITS + 1, mem_hbm, memory)
    load_lk = load(UNITS + 2, lk_hbm, keys.at[:, pl.ds(MEM, LEFT), :])
    load_lv = load(UNITS + 3, lv_hbm, values.at[:, pl.ds(MEM, LEFT), :])
    load_feat.start()
    for c in loads[:4]:
        c.start()
    load_mem.start()
    load_lk.start()
    load_lv.start()
    for c in loads[4:]:
        c.start()

    barrier = pltpu.get_barrier_semaphore()

    def greet(to):
        pl.semaphore_signal(
            barrier, inc=1, device_id=to, device_id_type=pl.DeviceIdType.MESH
        )

    def greet_sources(j, _):
        kk = 2 * j + m
        greet(dev(2 * kk + odd, f, 1 - lax.rem(k, 2)))
        return 0

    lax.fori_loop(0, 16, greet_sources, 0)

    def quad(e):
        s = lax.rem(slot + e, 8)
        rr = lax.div(s, 2)
        return rr, dev(2 * k + lax.div(rr, 2), lax.rem(rr, 2), lax.rem(s, 2))

    def greet_quad(e, _):
        greet(quad(e)[1])
        return 0

    lax.fori_loop(1, 8, greet_quad, 0)
    greet(cross_dev)
    for to in ring:
        greet(to)
    greet(sibling)
    pl.semaphore_wait(barrier, 16 + 7 + 1 + 3 + 1)

    def first_copy(j):
        t = 2 * lax.rem(j + lax.div(k, 2), 16) + (1 - m)
        return remote(
            feat.at[:, :, pl.ds(pl.multiple_of(t * 128, 128), 128)],
            gath.at[lax.div(k, 2)],
            g_send.at[j],
            g_recv.at[lax.div(k, 2)],
            dev(2 * t + odd, f, lax.rem(k, 2)),
        )

    def send_first(j, _):
        first_copy(j).start()
        return 0

    load_feat.wait()
    lax.fori_loop(0, 16, send_first, 0)

    def piece(ref, u, c):
        return ref.at[u, pl.ds(pl.multiple_of(c * 128, 128), 128), :]

    other = lax.rem(color + 2, 4)

    def cross_copy(u):
        return remote(
            piece(own, u, other), piece(got, u, other), c_send.at[u], c_recv.at[u], cross_dev
        )

    def forward_copy(u, i):
        return remote(
            piece(got, u, color), piece(got, u, color), f_send.at[u, i], f_recv.at[u, i], ring[i]
        )

    def wait_got(u, c, sem):
        pltpu.make_async_copy(piece(got, u, c), piece(got, u, c), sem).wait()

    def forward(u):
        wait_got(u, color, c_recv.at[u])
        for i in range(3):
            forward_copy(u, i).start()

    def ready(u):
        wait_got(u, lax.rem(color + 2, 4), f_recv.at[u, 0])
        wait_got(u, lax.rem(color + 3, 4), f_recv.at[u, 1])
        wait_got(u, lax.rem(color + 1, 4), f_recv.at[u, 2])

    for u in range(UNITS):
        loads[u].wait()
        cross_copy(u).start()

    def build_perm(s, _):
        at = lax.broadcasted_iota(jnp.int32, (128, 1024), 0)
        col = lax.broadcasted_iota(jnp.int32, (128, 1024), 1)
        want = (at >> 3) * 64 + lax.rem(s, 2) * 32 + lax.div(s, 2) * 8 + (at & 7)
        perm[pl.ds(pl.multiple_of(s * 128, 128), 128), :] = jnp.where(
            col == want, 1.0, 0.0
        ).astype(BF16)
        return 0

    lax.fori_loop(0, 8, build_perm, 0)
    at = lax.broadcasted_iota(jnp.int32, (STR * ROWS, STR * FRAMES), 0)
    col = lax.broadcasted_iota(jnp.int32, (STR * ROWS, STR * FRAMES), 1)
    rows[...] = jnp.where(col == (at & 7) * STR + (at >> 3), 1.0, 0.0).astype(BF16)
    att[...] = jnp.zeros_like(att)

    def wait_first(j, _):
        pltpu.make_async_copy(gath.at[j], gath.at[j], g_recv.at[j]).wait()
        return 0

    lax.fori_loop(0, 16, wait_first, 0)
    for fr in range(FRAMES):
        turned = gath[:, fr].astype(F32).reshape(128, 128).T.astype(BF16)
        blocks[:, fr] = turned.reshape(4, STR, 128)

    def second_copy(e):
        rr, to = quad(e)
        return remote(blocks.at[rr], held.at[slot], h_send.at[e], h_recv.at[slot], to)

    def send_second(e, _):
        second_copy(e).start()
        return 0

    lax.fori_loop(1, 8, send_second, 0)
    held[slot] = blocks[r]

    forward(0)
    forward(1)

    def wait_second(e, _):
        s = lax.rem(slot + e, 8)
        pltpu.make_async_copy(held.at[s], held.at[s], h_recv.at[s]).wait()
        return 0

    lax.fori_loop(1, 8, wait_second, 0)
    for s in range(8):
        xp[:, pl.ds(128 * s, 128)] = held[s].reshape(STR * FRAMES, 128)
    for h in range(2):
        half = pl.ds(512 * h, 512)
        placed = dot(xp[...], perm[:, half]).astype(BF16)
        x[:, half] = dot(rows[...], placed)

    def split_norm(values_f32, chunk):
        at = pl.ds(pl.multiple_of(chunk * 32, 32), 32)
        b = values_f32.astype(BF16)
        n[0, at, :] = b[:, :512]
        n[1, at, :] = b[:, 512:]

    def first_norm(c, _):
        at = pl.ds(pl.multiple_of(c * 32, 32), 32)
        v = normalized(x[at, :]).astype(BF16).astype(F32).reshape(4, ROWS, 1024)
        row = lax.broadcasted_iota(jnp.int32, v.shape, 1)
        summary = jnp.sum(jnp.where(row < GROUP, v, 0.0), axis=1, keepdims=True) * (1.0 / GROUP)
        v = jnp.where(row == FRAMES, summary, v)
        split_norm(v.reshape(32, 1024), c)
        return 0

    lax.fori_loop(0, 8, first_norm, 0)
    forward(2)

    load_mem.wait()
    load_lk.wait()
    load_lv.wait()

    mine = pl.ds(pl.multiple_of(f * 512, 512), 512)
    theirs = pl.ds(pl.multiple_of((1 - f) * 512, 512), 512)

    def project(u, place, center):
        def memory_rows(c, _):
            at = pl.ds(pl.multiple_of(c * 256, 256), 256)
            sums = dot(memory[at, mine], own[u]) + dot(memory[at, theirs], got[u])
            place[pl.ds(c * 8, 8), pl.ds(0, MEM), :] = sums.astype(BF16).reshape(8, MEM, 512)
            return 0

        lax.fori_loop(0, 4, memory_rows, 0)

        def group_rows(c, _):
            at = pl.ds(pl.multiple_of(c * 64, 64), 64)
            sums = dot(n[f, at, :], own[u]) + dot(n[1 - f, at, :], got[u])
            g = sums.reshape(8, ROWS, 512)
            both = jnp.concatenate([g, jnp.zeros_like(g)], axis=1).astype(BF16)
            place[pl.ds(c * 8, 8), pl.ds(MEM + LEFT, 16), :] = both
            center[pl.ds(c * 8, 8), :, :] = g[:, :GROUP, :].astype(BF16)
            return 0

        lax.fori_loop(0, 4, group_rows, 0)

    ready(0)
    project(0, keys, center_k)
    forward(3)
    ready(1)
    project(1, values, center_v)
    ready(2)
    q[...] = (
        (dot(n[f], own[2]) + dot(n[1 - f], got[2])).astype(BF16).astype(F32) * (HD**-0.5)
    ).reshape(STR, ROWS, 512)

    heads = ROWS
    head_mask = jnp.where(
        (lax.broadcasted_iota(jnp.int32, (heads, 512), 1) >> 6)
        == lax.broadcasted_iota(jnp.int32, (heads, 512), 0),
        1.0,
        0.0,
    )
    queries = FRAMES + 1

    def attend(s):
        q8 = q[s]
        spread = jnp.concatenate(
            [jnp.broadcast_to(q8[i : i + 1], (heads, 512)) * head_mask for i in range(queries)],
            axis=0,
        ).astype(BF16)
        scores = lax.dot_general(
            spread, keys[s], (((1,), (1,)), ((), ())), preferred_element_type=F32
        )
        row = lax.broadcasted_iota(jnp.int32, scores.shape, 0)
        col = lax.broadcasted_iota(jnp.int32, scores.shape, 1)
        seen_mem = (col >= MEM - fill[s]) & (col < MEM) & (row < FRAMES * heads)
        seen_left = (col >= MEM + LEFT - length[s]) & (col < MEM + LEFT + FRAMES)
        scores = jnp.where(seen_mem | seen_left, scores, MASKED)
        e = jnp.exp(scores - jnp.max(scores, axis=-1, keepdims=True))
        probs = (e / jnp.sum(e, axis=-1, keepdims=True)).astype(BF16)
        mixed = dot(probs, values[s]).reshape(queries, heads, 512)
        att[s, pl.ds(0, queries), :] = jnp.sum(mixed * head_mask[None], axis=1)

    def attend_block(b, _):
        forward(4 + b)

        def pair(i, _):
            attend(b * 8 + 2 * i)
            attend(b * 8 + 2 * i + 1)
            return 0

        lax.fori_loop(0, 4, pair, 0)
        return 0

    lax.fori_loop(0, 4, attend_block, 0)

    def exchange(src, dst, i):
        return remote(src, dst, e_send.at[i], e_recv.at[i], sibling)

    ready(3)
    a = att[...].reshape(STR * ROWS, 512).astype(BF16)
    part[f] = dot(a, own[3]).astype(BF16)
    part[1 - f] = dot(a, got[3]).astype(BF16)
    first = exchange(part, part_in, 0)
    first.start()
    first.wait()

    def second_norm(c, _):
        at = pl.ds(pl.multiple_of(c * 32, 32), 32)
        summed = [part[h, at, :].astype(F32) + part_in[h, at, :].astype(F32) for h in range(2)]
        v = x[at, :] + jnp.concatenate(summed, axis=1)
        x[at, :] = v
        split_norm(normalized(v), c)
        return 0

    lax.fori_loop(0, 8, second_norm, 0)
    mem_next[...] = jnp.tanh(x[...].reshape(STR, ROWS, 1024)[:, FRAMES, :]).astype(BF16)

    down[...] = jnp.zeros_like(down)

    def hidden_block(j, _):
        @pl.when(j < 2)
        def _():
            forward(8 + 2 * j)
            forward(9 + 2 * j)

        ready(4 + 2 * j)
        sums = dot(n[f], own[4 + 2 * j]) + dot(n[1 - f], got[4 + 2 * j])
        hid = jax.nn.gelu(sums, approximate=True).astype(BF16)
        ready(5 + 2 * j)
        down[f] += dot(hid, own[5 + 2 * j])
        down[1 - f] += dot(hid, got[5 + 2 * j])
        return 0

    lax.fori_loop(0, 4, hidden_block, 0)
    down_out[...] = down[...].astype(BF16)
    last = exchange(down_out, down_in, 1)
    last.start()
    last.wait()

    def third_norm(c, _):
        at = pl.ds(pl.multiple_of(c * 32, 32), 32)
        summed = [down_out[h, at, :].astype(F32) + down_in[h, at, :].astype(F32) for h in range(2)]
        v = x[at, :] + jnp.concatenate(summed, axis=1)
        w = (normalized(v) * gain[...]).reshape(4, ROWS, 1024)
        out[pl.ds(c * 4, 4), :, :] = w[:, :FRAMES, :].astype(BF16)
        return 0

    lax.fori_loop(0, 8, third_norm, 0)

    def drain_first(j, _):
        first_copy(j).wait_send()
        return 0

    lax.fori_loop(0, 16, drain_first, 0)

    def drain_second(e, _):
        second_copy(e).wait_send()
        return 0

    lax.fori_loop(1, 8, drain_second, 0)

    def drain(u, _):
        cross_copy(u).wait_send()
        for i in range(3):
            forward_copy(u, i).wait_send()
        return 0

    lax.fori_loop(0, UNITS, drain, 0)


def shards(
    features,
    memory_bank,
    memory_fill,
    left_keys,
    left_values,
    left_length,
    w_query,
    w_key,
    w_value,
    w_out,
    w_up,
    w_down,
    out_gain,
):
    memory = memory_bank.reshape(STR * MEM, 1024)
    smem = pl.BlockSpec(memory_space=pltpu.SMEM)
    hbm = pl.BlockSpec(memory_space=pl.ANY)
    vmem = pl.BlockSpec(memory_space=pltpu.VMEM)
    dma = pltpu.SemaphoreType.DMA
    return pl.pallas_call(
        kernel,
        name="layer",
        out_shape=(
            jax.ShapeDtypeStruct((STR, FRAMES, 1024), BF16),
            jax.ShapeDtypeStruct((STR, 1024), BF16),
            jax.ShapeDtypeStruct((STR, GROUP, 512), BF16),
            jax.ShapeDtypeStruct((STR, GROUP, 512), BF16),
        ),
        in_specs=[smem] * 2 + [hbm] * 10 + [vmem],
        out_specs=(vmem,) * 4,
        scratch_shapes=[
            pltpu.VMEM((FRAMES, 8, 4096), BF16),
            pltpu.VMEM((16, FRAMES, 8, 128), BF16),
            pltpu.VMEM((4, FRAMES, STR, 128), BF16),
            pltpu.VMEM((8, FRAMES, STR, 128), BF16),
            pltpu.VMEM((1024, 1024), BF16),
            pltpu.VMEM((STR * ROWS, STR * FRAMES), BF16),
            pltpu.VMEM((STR * FRAMES, 1024), BF16),
            pltpu.VMEM((STR * ROWS, 1024), F32),
            pltpu.VMEM((2, STR * ROWS, 512), BF16),
            pltpu.VMEM((UNITS, 512, 512), BF16),
            pltpu.VMEM((UNITS, 512, 512), BF16),
            pltpu.VMEM((STR * MEM, 1024), BF16),
            pltpu.VMEM((STR, KEYS, 512), BF16),
            pltpu.VMEM((STR, KEYS, 512), BF16),
            pltpu.VMEM((STR, ROWS, 512), F32),
            pltpu.VMEM((STR, ROWS, 512), F32),
            pltpu.VMEM((2, STR * ROWS, 512), BF16),
            pltpu.VMEM((2, STR * ROWS, 512), BF16),
            pltpu.VMEM((2, STR * ROWS, 512), F32),
            pltpu.VMEM((2, STR * ROWS, 512), BF16),
            pltpu.VMEM((2, STR * ROWS, 512), BF16),
            dma((UNITS + 4,)),
            dma((16,)),
            dma((16,)),
            dma((8,)),
            dma((8,)),
            dma((UNITS,)),
            dma((UNITS,)),
            dma((UNITS, 3)),
            dma((UNITS, 3)),
            dma((2,)),
            dma((2,)),
        ],
        compiler_params=pltpu.CompilerParams(
            collective_id=0, has_side_effects=True, vmem_limit_bytes=60 * 1024 * 1024
        ),
    )(
        memory_fill,
        left_length,
        features,
        memory,
        left_keys,
        left_values,
        w_query,
        w_key,
        w_value,
        w_out,
        w_up,
        w_down,
        out_gain.reshape(1, 1024),
    )


def solution(mesh):
    in_specs = (
        P(None, ("dp", "fsdp"), None),
        P(("dp", "fsdp"), None, None),
        P(("dp", "fsdp")),
        P(("dp", "fsdp"), None, "mp"),
        P(("dp", "fsdp"), None, "mp"),
        P(("dp", "fsdp")),
        P("fsdp", "mp"),
        P("fsdp", "mp"),
        P("fsdp", "mp"),
        P("mp", "fsdp"),
        P("fsdp", "mp"),
        P("mp", "fsdp"),
        P(),
    )
    out_specs = (
        P(("dp", "fsdp"), None, None),
        P(("dp", "fsdp"), None),
        P(("dp", "fsdp"), None, "mp"),
        P(("dp", "fsdp"), None, "mp"),
    )
    return jax.shard_map(shards, mesh=mesh, in_specs=in_specs, out_specs=out_specs, check_vma=False)
```

```python
import functools

import jax
import jax.numpy as jnp
from jax import lax
from jax.experimental import pallas as pl
from jax.experimental.pallas import tpu as pltpu
from jax.sharding import PartitionSpec as P

HD = 64
GROUP = 4
FRAMES = 5
MEM = 32
LEFT = 64
STR = 32
ROWS = 8
KEYS = 112
UNITS = 12
DIRECT = 8
ORDER = (0, 1, 2, 8, 9, 3, 10, 11, 4, 5, 6, 7)
EPS = 1e-05
MASKED = -1e30
F32 = jnp.float32
BF16 = jnp.bfloat16


def dot(a, b):
    return jnp.dot(a, b, preferred_element_type=F32)


def normalized(x):
    mean = jnp.sum(x, axis=-1, keepdims=True) * (1.0 / x.shape[-1])
    cent = x - mean
    var = jnp.sum(cent * cent, axis=-1, keepdims=True) * (1.0 / x.shape[-1])
    return cent * lax.rsqrt(var + EPS)


def kernel(
    fill,
    length,
    feat_hbm,
    mem_hbm,
    lk_hbm,
    lv_hbm,
    wq_hbm,
    wk_hbm,
    wv_hbm,
    wo_hbm,
    wu_hbm,
    wd_hbm,
    gain,
    out,
    mem_next,
    center_k,
    center_v,
    feat,
    gath,
    blocks,
    held,
    perm,
    rows,
    frames_first,
    xp,
    x,
    n,
    own,
    got,
    memory,
    keys,
    values,
    q,
    att,
    part,
    part_in,
    down,
    down_out,
    down_in,
    k_half,
    v_half,
    l_sem,
    g_send,
    g_recv,
    h_send,
    h_recv,
    c_send,
    c_recv,
    f_send,
    f_recv,
    z_send,
    z_recv,
    e_send,
    e_recv,
):
    d = lax.axis_index("dp")
    m = lax.axis_index("mp")
    f = lax.axis_index("fsdp")
    xl = lax.div(d, 32)
    y = lax.rem(lax.div(d, 8), 4)
    z = lax.rem(d, 8)
    k = lax.div(d, 2)
    odd = lax.rem(d, 2)
    r = odd * 2 + f
    slot = r * 2 + m
    color = lax.rem(y + 2 * xl, 4)

    def dev(dd, ff, mm):
        return {"dp": dd, "fsdp": ff, "mp": mm}

    def remote(src, dst, send, recv, to):
        return pltpu.make_async_remote_copy(
            src_ref=src,
            dst_ref=dst,
            send_sem=send,
            recv_sem=recv,
            device_id=to,
            device_id_type=pl.DeviceIdType.MESH,
        )

    flipped = d + 32 * (1 - 2 * xl)
    over = lax.div(flipped, 2)
    z_up = dev(d - z + lax.rem(z + 1, 8), f, m)
    z_down = dev(d - z + lax.rem(z + 7, 8), f, m)
    up_d = xl * 32 + lax.rem(y + 1, 4) * 8 + z
    down_d = xl * 32 + lax.rem(y + 3, 4) * 8 + z
    cross_dev = dev(flipped, 1 - f, m)
    ring = (dev(flipped, f, m), dev(up_d, f, m), dev(down_d, f, m))
    sibling = dev(d, f, 1 - m)

    def load(i, src, dst):
        return pltpu.make_async_copy(src, dst, l_sem.at[i])

    units = [wk_hbm, wv_hbm, wq_hbm, wo_hbm]
    for j in range(4):
        units.append(wu_hbm.at[:, pl.ds(512 * j, 512)])
        units.append(wd_hbm.at[pl.ds(512 * j, 512), :])
    loads = [load(u, units[u], own.at[u]) for u in range(UNITS)]
    load_feat = load(UNITS, feat_hbm, feat)
    load_mem = load(UNITS + 1, mem_hbm, memory)
    load_lk = load(UNITS + 2, lk_hbm, keys.at[:, pl.ds(MEM, LEFT), :])
    load_lv = load(UNITS + 3, lv_hbm, values.at[:, pl.ds(MEM, LEFT), :])
    load_feat.start()
    loads[0].start()
    load_mem.start()
    for u in ORDER[1:]:
        loads[u].start()
    load_lk.start()
    load_lv.start()

    barrier = pltpu.get_barrier_semaphore()

    def greet(to):
        pl.semaphore_signal(
            barrier, inc=1, device_id=to, device_id_type=pl.DeviceIdType.MESH
        )

    def greet_sources(j, _):
        kk = 2 * j + m
        greet(dev(2 * kk + odd, f, 1 - lax.rem(k, 2)))
        return 0

    lax.fori_loop(0, 16, greet_sources, 0)

    def quad(e):
        s = lax.rem(slot + e, 8)
        rr = lax.div(s, 2)
        return rr, dev(2 * over + lax.div(rr, 2), lax.rem(rr, 2), lax.rem(s, 2))

    def greet_quad(e, _):
        greet(quad(e)[1])
        return 0

    lax.fori_loop(0, 8, greet_quad, 0)
    greet(cross_dev)
    for to in ring:
        greet(to)
    greet(sibling)
    greet(z_up)
    greet(z_down)

    def build_perm(s, _):
        at = lax.broadcasted_iota(jnp.int32, (128, 1024), 0)
        col = lax.broadcasted_iota(jnp.int32, (128, 1024), 1)
        want = (at >> 3) * 64 + lax.rem(s, 2) * 32 + lax.div(s, 2) * 8 + (at & 7)
        perm[pl.ds(pl.multiple_of(s * 128, 128), 128), :] = jnp.where(
            col == want, 1.0, 0.0
        ).astype(BF16)
        return 0

    lax.fori_loop(0, 8, build_perm, 0)
    at = lax.broadcasted_iota(jnp.int32, (STR * ROWS, STR * FRAMES), 0)
    col = lax.broadcasted_iota(jnp.int32, (STR * ROWS, STR * FRAMES), 1)
    rows[...] = jnp.where(col == (at & 7) * STR + (at >> 3), 1.0, 0.0).astype(BF16)
    at = lax.broadcasted_iota(jnp.int32, (STR * FRAMES, STR * ROWS), 0)
    col = lax.broadcasted_iota(jnp.int32, (STR * FRAMES, STR * ROWS), 1)
    frames_first[...] = jnp.where(col == (at & 31) * ROWS + (at >> 5), 1.0, 0.0).astype(BF16)
    att[...] = jnp.zeros_like(att)

    mine = pl.ds(pl.multiple_of(f * 512, 512), 512)
    theirs = pl.ds(pl.multiple_of((1 - f) * 512, 512), 512)

    def own_half(u, place):
        def memory_rows(c, _):
            at = pl.ds(pl.multiple_of(c * 256, 256), 256)
            place[at, :] = dot(memory[at, mine], own[u])
            return 0

        lax.fori_loop(0, 4, memory_rows, 0)

    loads[0].wait()
    load_mem.wait()
    own_half(0, k_half)
    pl.semaphore_wait(barrier, 16 + 8 + 1 + 3 + 1 + 2)

    def first_copy(j):
        t = 2 * lax.rem(j + lax.div(over, 2), 16) + (1 - m)
        return remote(
            feat.at[:, :, pl.ds(pl.multiple_of(t * 128, 128), 128)],
            gath.at[lax.div(k, 2)],
            g_send.at[j],
            g_recv.at[lax.div(k, 2)],
            dev(lax.rem(2 * t + 32, 64) + odd, f, lax.rem(k, 2)),
        )

    def send_first(j, _):
        first_copy(j).start()
        return 0

    load_feat.wait()
    lax.fori_loop(0, 16, send_first, 0)

    def piece(ref, u, c):
        return ref.at[u, pl.ds(pl.multiple_of(c * 128, 128), 128), :]

    def eighth(ref, u, step):
        c = lax.rem(z + 8 + step, 8)
        return ref.at[u, pl.ds(pl.multiple_of(c * 64, 64), 64), :]

    def sixteenth(ref, u, step, half):
        c = lax.rem(z + 8 + step, 8)
        return ref.at[u, pl.ds(pl.multiple_of(c * 64 + 32 * half, 32), 32), :]

    other = lax.rem(color + 2, 4)

    def cross_copy(u):
        if u < DIRECT:
            src, dst = piece(own, u, other), piece(got, u, other)
        else:
            src, dst = eighth(own, u, 0), eighth(got, u, 0)
        return remote(src, dst, c_send.at[u], c_recv.at[u], cross_dev)

    def forward_copy(u, i):
        return remote(
            piece(got, u, color), piece(got, u, color), f_send.at[u, i], f_recv.at[u, i], ring[i]
        )

    def ring_copy(u, step, way):
        sign = 1 - 2 * way
        if step < 3:
            at = eighth(got, u, -sign * step)
        else:
            at = sixteenth(got, u, -sign * step, way)
        sems = z_send.at[u - DIRECT, step, way], z_recv.at[u - DIRECT, step, way]
        return remote(at, at, *sems, (z_up, z_down)[way])

    def arrived(ref, sem):
        pltpu.make_async_copy(ref, ref, sem).wait()

    def forward(u):
        arrived(piece(got, u, color), c_recv.at[u])
        for i in range(3):
            forward_copy(u, i).start()

    def ring_arrived(u, step, way):
        sign = 1 - 2 * way
        if step < 3:
            at = eighth(got, u, -sign * (step + 1))
        else:
            at = sixteenth(got, u, -sign * (step + 1), way)
        arrived(at, z_recv.at[u - DIRECT, step, way])

    def circulate(u, step):
        for way in range(2):
            if step > 0:
                ring_arrived(u, step - 1, way)
            elif way == 0:
                arrived(eighth(got, u, 0), c_recv.at[u])
            ring_copy(u, step, way).start()

    def ready(u):
        if u < DIRECT:
            for i, c in enumerate((2, 3, 1)):
                arrived(piece(got, u, lax.rem(color + c, 4)), f_recv.at[u, i])
        else:
            for way in range(2):
                ring_arrived(u, 3, way)

    def across(units):
        for u in units:
            if u > 0:
                loads[u].wait()
            cross_copy(u).start()

    across(ORDER[:2])
    own_half(1, v_half)

    def wait_first(j, _):
        pltpu.make_async_copy(gath.at[j], gath.at[j], g_recv.at[j]).wait()
        return 0

    lax.fori_loop(0, 16, wait_first, 0)
    for fr in range(FRAMES):
        turned = gath[:, fr].astype(F32).reshape(128, 128).T.astype(BF16)
        blocks[:, fr] = turned.reshape(4, STR, 128)

    def second_copy(e):
        rr, to = quad(e)
        return remote(blocks.at[rr], held.at[slot], h_send.at[e], h_recv.at[slot], to)

    def send_second(e, _):
        second_copy(e).start()
        return 0

    lax.fori_loop(0, 8, send_second, 0)

    across(ORDER[2:])
    forward(0)
    forward(1)

    def wait_second(e, _):
        s = lax.rem(slot + e, 8)
        pltpu.make_async_copy(held.at[s], held.at[s], h_recv.at[s]).wait()
        return 0

    lax.fori_loop(0, 8, wait_second, 0)
    for s in range(8):
        xp[:, pl.ds(128 * s, 128)] = held[s].reshape(STR * FRAMES, 128)
    for h in range(2):
        half = pl.ds(512 * h, 512)
        placed = dot(xp[...], perm[:, half]).astype(BF16)
        x[:, half] = dot(rows[...], placed)

    def split_norm(values_f32, chunk):
        at = pl.ds(pl.multiple_of(chunk * 32, 32), 32)
        b = values_f32.astype(BF16)
        n[0, at, :] = b[:, :512]
        n[1, at, :] = b[:, 512:]

    def first_norm(c, _):
        at = pl.ds(pl.multiple_of(c * 32, 32), 32)
        v = normalized(x[at, :]).astype(BF16).astype(F32).reshape(4, ROWS, 1024)
        row = lax.broadcasted_iota(jnp.int32, v.shape, 1)
        summary = jnp.sum(jnp.where(row < GROUP, v, 0.0), axis=1, keepdims=True) * (1.0 / GROUP)
        v = jnp.where(row == FRAMES, summary, v)
        split_norm(v.reshape(32, 1024), c)
        return 0

    lax.fori_loop(0, 8, first_norm, 0, unroll=4)
    forward(2)
    circulate(8, 0)

    load_lk.wait()
    load_lv.wait()

    def project(u, half, place, center):
        def memory_rows(c, _):
            at = pl.ds(pl.multiple_of(c * 256, 256), 256)
            sums = half[at, :] + dot(memory[at, theirs], got[u])
            place[pl.ds(c * 8, 8), pl.ds(0, MEM), :] = sums.astype(BF16).reshape(8, MEM, 512)
            return 0

        lax.fori_loop(0, 4, memory_rows, 0)

        def group_rows(c, _):
            at = pl.ds(pl.multiple_of(c * 64, 64), 64)
            sums = dot(n[f, at, :], own[u]) + dot(n[1 - f, at, :], got[u])
            g = sums.reshape(8, ROWS, 512)
            both = jnp.concatenate([g, jnp.zeros_like(g)], axis=1).astype(BF16)
            place[pl.ds(c * 8, 8), pl.ds(MEM + LEFT, 16), :] = both
            center[pl.ds(c * 8, 8), :, :] = g[:, :GROUP, :].astype(BF16)
            return 0

        lax.fori_loop(0, 4, group_rows, 0)

    ready(0)
    project(0, k_half, keys, center_k)
    circulate(9, 0)
    ready(1)
    project(1, v_half, values, center_v)
    forward(3)
    circulate(8, 1)
    ready(2)
    q[...] = (
        (dot(n[f], own[2]) + dot(n[1 - f], got[2])).astype(BF16).astype(F32) * (HD**-0.5)
    ).reshape(STR, ROWS, 512)

    heads = ROWS
    head_mask = jnp.where(
        (lax.broadcasted_iota(jnp.int32, (heads, 512), 1) >> 6)
        == lax.broadcasted_iota(jnp.int32, (heads, 512), 0),
        1.0,
        0.0,
    )
    queries = FRAMES + 1

    width = 4

    def attend(first):
        streams = [first + i for i in range(width)]
        probs = []
        scored = []
        for s in streams:
            q8 = q[s]
            spread = jnp.concatenate(
                [
                    jnp.broadcast_to(q8[i : i + 1], (heads, 512)) * head_mask
                    for i in range(queries)
                ],
                axis=0,
            ).astype(BF16)
            scored.append(
                lax.dot_general(
                    spread, keys[s], (((1,), (1,)), ((), ())), preferred_element_type=F32
                )
            )
        row = lax.broadcasted_iota(jnp.int32, (queries * heads, KEYS), 0)
        col = lax.broadcasted_iota(jnp.int32, (queries * heads, KEYS), 1)
        in_mem = (col < MEM) & (row < FRAMES * heads)
        in_rest = col < MEM + LEFT + FRAMES
        for s, scores in zip(streams, scored):
            seen_mem = (col >= MEM - fill[s]) & in_mem
            seen_left = (col >= MEM + LEFT - length[s]) & in_rest
            scores = jnp.where(seen_mem | seen_left, scores, MASKED)
            e = jnp.exp(scores - jnp.max(scores, axis=-1, keepdims=True))
            probs.append((e / jnp.sum(e, axis=-1, keepdims=True)).astype(BF16))
        for s, p in zip(streams, probs):
            mixed = dot(p, values[s]).reshape(queries, heads, 512)
            att[s, pl.ds(0, queries), :] = jnp.sum(mixed * head_mask[None], axis=1)

    def attend_block(b):
        def few(i, _):
            attend(b * 8 + width * i)
            return 0

        lax.fori_loop(0, 8 // width, few, 0)

    circulate(9, 1)
    circulate(10, 0)
    attend_block(0)
    circulate(8, 2)
    circulate(11, 0)
    attend_block(1)
    circulate(9, 2)
    attend_block(2)
    circulate(10, 1)
    forward(4)
    attend_block(3)

    def exchange(src, dst, i):
        return remote(src, dst, e_send.at[i], e_recv.at[i], sibling)

    ready(3)
    a = att[...].reshape(STR * ROWS, 512).astype(BF16)
    part[f] = dot(a, own[3]).astype(BF16)
    exchange(part.at[f], part_in.at[f], 0).start()
    part[1 - f] = dot(a, got[3]).astype(BF16)
    exchange(part.at[1 - f], part_in.at[1 - f], 1).start()
    circulate(8, 3)
    circulate(11, 1)
    exchange(part.at[f], part_in.at[f], 0).wait()
    exchange(part.at[1 - f], part_in.at[1 - f], 1).wait()

    def second_norm(c, _):
        at = pl.ds(pl.multiple_of(c * 32, 32), 32)
        summed = [part[h, at, :].astype(F32) + part_in[h, at, :].astype(F32) for h in range(2)]
        v = x[at, :] + jnp.concatenate(summed, axis=1)
        x[at, :] = v
        split_norm(normalized(v), c)
        return 0

    lax.fori_loop(0, 8, second_norm, 0, unroll=4)
    circulate(9, 3)
    forward(5)
    mem_next[...] = jnp.tanh(x[...].reshape(STR, ROWS, 1024)[:, FRAMES, :]).astype(BF16)

    def hidden_block(u, pumps):
        ready(u)
        sums = dot(n[f], own[u]) + dot(n[1 - f], got[u])
        hid = jax.nn.gelu(sums, approximate=True).astype(BF16)
        for pump in pumps:
            pump()
        ready(u + 1)
        return hid

    def pump(u, step=None):
        return functools.partial(forward, u) if step is None else functools.partial(circulate, u, step)

    hid = hidden_block(8, (pump(10, 2),))
    down[f] = dot(hid, own[9])
    down[1 - f] = dot(hid, got[9])
    circulate(11, 2)
    forward(6)
    hid = hidden_block(4, (pump(10, 3),))
    down[f] += dot(hid, own[5])
    down[1 - f] += dot(hid, got[5])
    circulate(11, 3)
    forward(7)
    hid = hidden_block(10, ())
    down[f] += dot(hid, own[11])
    down[1 - f] += dot(hid, got[11])
    hid = hidden_block(6, ())
    down_out[f] = (down[f] + dot(hid, own[7])).astype(BF16)
    exchange(down_out.at[f], down_in.at[f], 2).start()
    down_out[1 - f] = (down[1 - f] + dot(hid, got[7])).astype(BF16)
    exchange(down_out.at[1 - f], down_in.at[1 - f], 3).start()
    exchange(down_out.at[f], down_in.at[f], 2).wait()
    exchange(down_out.at[1 - f], down_in.at[1 - f], 3).wait()

    def third_norm(c, _):
        at = pl.ds(pl.multiple_of(c * 32, 32), 32)
        summed = [down_out[h, at, :].astype(F32) + down_in[h, at, :].astype(F32) for h in range(2)]
        v = x[at, :] + jnp.concatenate(summed, axis=1)
        split_norm(normalized(v) * gain[...], c)
        return 0

    lax.fori_loop(0, 8, third_norm, 0, unroll=4)
    for h in range(2):
        placed = dot(frames_first[...], n[h]).astype(BF16)
        out[:, :, pl.ds(512 * h, 512)] = placed.reshape(FRAMES, STR, 512)

    def drain_first(j, _):
        first_copy(j).wait_send()
        return 0

    lax.fori_loop(0, 16, drain_first, 0)

    def drain_second(e, _):
        second_copy(e).wait_send()
        return 0

    lax.fori_loop(0, 8, drain_second, 0)

    for u in range(UNITS):
        cross_copy(u).wait_send()
        if u < DIRECT:
            for i in range(3):
                forward_copy(u, i).wait_send()
        else:
            for step in range(4):
                for way in range(2):
                    ring_copy(u, step, way).wait_send()


def hand_over(*refs):
    given, held, results, into, out_of = refs[:4], refs[4:8], refs[8:12], refs[12], refs[13]
    arrive = [
        pltpu.make_async_copy(*pair, into.at[i]) for i, pair in enumerate(zip(given, results))
    ]
    leave = [
        pltpu.make_async_copy(*pair, out_of.at[i]) for i, pair in enumerate(zip(results, held))
    ]
    for copy in arrive:
        copy.start()
    for i in range(4):
        arrive[i].wait()
        leave[i].start()
    for copy in leave:
        copy.wait()


def shards(
    features,
    memory_bank,
    memory_fill,
    left_keys,
    left_values,
    left_length,
    w_query,
    w_key,
    w_value,
    w_out,
    w_up,
    w_down,
    out_gain,
):
    memory = memory_bank.reshape(STR * MEM, 1024)
    smem = pl.BlockSpec(memory_space=pltpu.SMEM)
    hbm = pl.BlockSpec(memory_space=pltpu.HBM)
    vmem = pl.BlockSpec(memory_space=pltpu.VMEM)
    dma = pltpu.SemaphoreType.DMA
    shapes = (
        jax.ShapeDtypeStruct((FRAMES, STR, 1024), BF16),
        jax.ShapeDtypeStruct((STR, 1024), BF16),
        jax.ShapeDtypeStruct((STR, GROUP, 512), BF16),
        jax.ShapeDtypeStruct((STR, GROUP, 512), BF16),
    )
    results = pl.pallas_call(
        kernel,
        name="layer",
        out_shape=shapes,
        in_specs=[smem] * 2 + [hbm] * 10 + [vmem],
        out_specs=(vmem,) * 4,
        scratch_shapes=[
            pltpu.VMEM((FRAMES, 8, 4096), BF16),
            pltpu.VMEM((16, FRAMES, 8, 128), BF16),
            pltpu.VMEM((4, FRAMES, STR, 128), BF16),
            pltpu.VMEM((8, FRAMES, STR, 128), BF16),
            pltpu.VMEM((1024, 1024), BF16),
            pltpu.VMEM((STR * ROWS, STR * FRAMES), BF16),
            pltpu.VMEM((STR * FRAMES, STR * ROWS), BF16),
            pltpu.VMEM((STR * FRAMES, 1024), BF16),
            pltpu.VMEM((STR * ROWS, 1024), F32),
            pltpu.VMEM((2, STR * ROWS, 512), BF16),
            pltpu.VMEM((UNITS, 512, 512), BF16),
            pltpu.VMEM((UNITS, 512, 512), BF16),
            pltpu.VMEM((STR * MEM, 1024), BF16),
            pltpu.VMEM((STR, KEYS, 512), BF16),
            pltpu.VMEM((STR, KEYS, 512), BF16),
            pltpu.VMEM((STR, ROWS, 512), F32),
            pltpu.VMEM((STR, ROWS, 512), F32),
            pltpu.VMEM((2, STR * ROWS, 512), BF16),
            pltpu.VMEM((2, STR * ROWS, 512), BF16),
            pltpu.VMEM((2, STR * ROWS, 512), F32),
            pltpu.VMEM((2, STR * ROWS, 512), BF16),
            pltpu.VMEM((2, STR * ROWS, 512), BF16),
            pltpu.VMEM((STR * MEM, 512), F32),
            pltpu.VMEM((STR * MEM, 512), F32),
            dma((UNITS + 4,)),
            dma((16,)),
            dma((16,)),
            dma((8,)),
            dma((8,)),
            dma((UNITS,)),
            dma((UNITS,)),
            dma((DIRECT, 3)),
            dma((DIRECT, 3)),
            dma((UNITS - DIRECT, 4, 2)),
            dma((UNITS - DIRECT, 4, 2)),
            dma((4,)),
            dma((4,)),
        ],
        compiler_params=pltpu.CompilerParams(
            collective_id=0, has_side_effects=True, vmem_limit_bytes=62_600_000
        ),
    )(
        memory_fill,
        left_length,
        features,
        memory,
        left_keys,
        left_values,
        w_query,
        w_key,
        w_value,
        w_out,
        w_up,
        w_down,
        out_gain.reshape(1, 1024),
    )
    layer_out, memory_next, center_keys, center_values = pl.pallas_call(
        hand_over,
        name="hand_over",
        out_shape=shapes,
        in_specs=[hbm] * 4,
        out_specs=(hbm,) * 4,
        scratch_shapes=[pltpu.VMEM(v.shape, v.dtype) for v in shapes] + [dma((4,)), dma((4,))],
        compiler_params=pltpu.CompilerParams(vmem_limit_bytes=62_600_000),
    )(*results)
    return jnp.transpose(layer_out, (1, 0, 2)), memory_next, center_keys, center_values


def solution(mesh):
    in_specs = (
        P(None, ("dp", "fsdp"), None),
        P(("dp", "fsdp"), None, None),
        P(("dp", "fsdp")),
        P(("dp", "fsdp"), None, "mp"),
        P(("dp", "fsdp"), None, "mp"),
        P(("dp", "fsdp")),
        P("fsdp", "mp"),
        P("fsdp", "mp"),
        P("fsdp", "mp"),
        P("mp", "fsdp"),
        P("fsdp", "mp"),
        P("mp", "fsdp"),
        P(),
    )
    out_specs = (
        P(("dp", "fsdp"), None, None),
        P(("dp", "fsdp"), None),
        P(("dp", "fsdp"), None, "mp"),
        P(("dp", "fsdp"), None, "mp"),
    )
    return jax.shard_map(shards, mesh=mesh, in_specs=in_specs, out_specs=out_specs, check_vma=False)
```

```python
import functools

import jax
import jax.numpy as jnp
from jax import lax
from jax.experimental import pallas as pl
from jax.experimental.pallas import tpu as pltpu
from jax.sharding import PartitionSpec as P

HD = 64
GROUP = 4
FRAMES = 5
MEM = 32
LEFT = 64
STR = 32
ROWS = 8
KEYS = 112
UNITS = 12
KIND = (1, 1, 1, 1, 2, 2, 1, 0, 2, 0, 0, 0)
ORDER = (1, 0, 2, 6, 3, 4, 5, 8, 7, 10, 11, 9)
EARLY = 4
BLOCKS = (3, 1, 0, 2)
STEPS = (
    ("own_v", 0),
    ("forward", 1),
    ("turn", 0),
    ("forward", 0),
    ("forward", 2),
    ("second", 1),
    ("forward", 6),
    ("relay", 0),
    ("second", 0),
    ("forward", 3),
    ("norm", 0),
    ("second", 2),
    ("circulate", 4, 0),
    ("second", 6),
    ("mem_v", 0),
    ("circulate", 5, 0),
    ("group_v", 0),
    ("second", 3),
    ("circulate", 8, 0),
    ("mem_k", 0),
    ("circulate", 4, 1),
    ("group_k", 0),
    ("forward", 7),
    ("circulate", 5, 1),
    ("query", 0),
    ("attend", 0),
    ("circulate", 8, 1),
    ("attend", 1),
    ("forward", 10),
    ("circulate", 4, 2),
    ("attend", 2),
    ("circulate", 5, 2),
    ("attend", 3),
    ("forward", 11),
    ("output", 0),
    ("circulate", 8, 2),
    ("circulate", 4, 3),
    ("norm_two", 0),
    ("forward", 9),
    ("next", 0),
    ("circulate", 5, 3),
    ("hidden", 3),
    ("circulate", 8, 3),
    ("down", 3),
    ("hidden", 1),
    ("down", 1),
    ("hidden", 0),
    ("down", 0),
    ("hidden", 2),
    ("down", 2),
    ("finish", 0),
)
EPS = 1e-05
MASKED = -1e30
F32 = jnp.float32
BF16 = jnp.bfloat16


def dot(a, b):
    return jnp.dot(a, b, preferred_element_type=F32)


def normalized(x):
    mean = jnp.sum(x, axis=-1, keepdims=True) * (1.0 / x.shape[-1])
    cent = x - mean
    var = jnp.sum(cent * cent, axis=-1, keepdims=True) * (1.0 / x.shape[-1])
    return cent * lax.rsqrt(var + EPS)


def kernel(
    fill,
    length,
    feat_hbm,
    mem_hbm,
    lk_hbm,
    lv_hbm,
    wq_hbm,
    wk_hbm,
    wv_hbm,
    wo_hbm,
    wu_hbm,
    wd_hbm,
    gain,
    out,
    mem_next,
    center_k,
    center_v,
    feat,
    gath,
    blocks,
    held,
    perm,
    rows,
    frames_first,
    xp,
    x,
    n,
    own,
    got,
    memory,
    keys,
    values,
    q,
    att,
    part,
    part_in,
    down,
    down_out,
    down_in,
    k_half,
    v_half,
    out_vm,
    mem_vm,
    ck_vm,
    cv_vm,
    o_sem,
    l_sem,
    sent,
    g_recv,
    h_recv,
    c_recv,
    s_recv,
    f_recv,
    z_recv,
    e_send,
    e_recv,
):
    d = lax.axis_index("dp")
    m = lax.axis_index("mp")
    f = lax.axis_index("fsdp")
    xl = lax.div(d, 32)
    y = lax.rem(lax.div(d, 8), 4)
    z = lax.rem(d, 8)
    k = lax.div(d, 2)
    odd = lax.rem(d, 2)
    r = odd * 2 + f
    color = lax.rem(y + 2 * xl, 4)

    def dev(dd, ff, mm):
        return {"dp": dd, "fsdp": ff, "mp": mm}

    def remote(src, dst, send, recv, to):
        return pltpu.make_async_remote_copy(
            src_ref=src,
            dst_ref=dst,
            send_sem=send,
            recv_sem=recv,
            device_id=to,
            device_id_type=pl.DeviceIdType.MESH,
        )

    flipped = d + 32 * (1 - 2 * xl)
    over = lax.div(flipped, 2)
    z_up = dev(d - z + lax.rem(z + 1, 8), f, m)
    z_down = dev(d - z + lax.rem(z + 7, 8), f, m)
    z_pair = dev(d + 1 - 2 * odd, f, m)
    up_d = xl * 32 + lax.rem(y + 1, 4) * 8 + z
    down_d = xl * 32 + lax.rem(y + 3, 4) * 8 + z
    cross_dev = dev(flipped, 1 - f, m)
    ring = (dev(flipped, f, m), dev(up_d, f, m), dev(down_d, f, m))
    sibling = dev(d, f, 1 - m)

    write = [
        pltpu.make_async_copy(src, dst, o_sem.at[i])
        for i, (src, dst) in enumerate(
            ((out_vm, out), (mem_vm, mem_next), (ck_vm, center_k), (cv_vm, center_v))
        )
    ]

    def load(i, src, dst):
        return pltpu.make_async_copy(src, dst, l_sem.at[i])

    units = [wk_hbm, wv_hbm, wq_hbm, wo_hbm]
    for j in range(4):
        units.append(wu_hbm.at[:, pl.ds(512 * j, 512)])
        units.append(wd_hbm.at[pl.ds(512 * j, 512), :])
    loads = [load(u, units[u], own.at[u]) for u in range(UNITS)]
    load_feat = load(UNITS, feat_hbm, feat)
    load_mem = load(UNITS + 1, mem_hbm, memory)
    load_lk = load(UNITS + 2, lk_hbm, keys.at[:, pl.ds(MEM, LEFT), :])
    load_lv = load(UNITS + 3, lv_hbm, values.at[:, pl.ds(MEM, LEFT), :])
    load_feat.start()
    loads[0].start()
    load_mem.start()
    for u in ORDER:
        if u > 0:
            loads[u].start()
    load_lk.start()
    load_lv.start()

    barrier = pltpu.get_barrier_semaphore()

    def greet(to):
        pl.semaphore_signal(
            barrier, inc=1, device_id=to, device_id_type=pl.DeviceIdType.MESH
        )

    def greet_sources(j, _):
        kk = 2 * j + m
        greet(dev(2 * kk + odd, f, 1 - lax.rem(k, 2)))
        return 0

    lax.fori_loop(0, 16, greet_sources, 0)

    def quad(e):
        rr = lax.rem(r + e, 4)
        return rr, dev(2 * over + lax.div(rr, 2), lax.rem(rr, 2), m)

    def greet_quad(e, _):
        greet(quad(e)[1])
        return 0

    lax.fori_loop(0, 4, greet_quad, 0)
    greet(cross_dev)
    for to in ring:
        greet(to)
    greet(sibling)
    greet(z_up)
    greet(z_down)
    greet(z_pair)

    def build_perm(s, _):
        at = lax.broadcasted_iota(jnp.int32, (128, 1024), 0)
        col = lax.broadcasted_iota(jnp.int32, (128, 1024), 1)
        want = (at >> 3) * 64 + lax.div(s, 4) * 32 + lax.rem(s, 4) * 8 + (at & 7)
        perm[pl.ds(pl.multiple_of(s * 128, 128), 128), :] = jnp.where(
            col == want, 1.0, 0.0
        ).astype(BF16)
        return 0

    lax.fori_loop(0, 8, build_perm, 0)
    at = lax.broadcasted_iota(jnp.int32, (STR * ROWS, STR * FRAMES), 0)
    col = lax.broadcasted_iota(jnp.int32, (STR * ROWS, STR * FRAMES), 1)
    rows[...] = jnp.where(col == (at & 7) * STR + (at >> 3), 1.0, 0.0).astype(BF16)
    at = lax.broadcasted_iota(jnp.int32, (STR * FRAMES, STR * ROWS), 0)
    col = lax.broadcasted_iota(jnp.int32, (STR * FRAMES, STR * ROWS), 1)
    frames_first[...] = jnp.where(col == (at & 31) * ROWS + (at >> 5), 1.0, 0.0).astype(BF16)
    att[...] = jnp.zeros_like(att)

    mine = pl.ds(pl.multiple_of(f * 512, 512), 512)
    theirs = pl.ds(pl.multiple_of((1 - f) * 512, 512), 512)

    def own_half(u, place):
        def memory_rows(c, _):
            at = pl.ds(pl.multiple_of(c * 256, 256), 256)
            place[at, :] = dot(memory[at, mine], own[u])
            return 0

        lax.fori_loop(0, 4, memory_rows, 0)

    loads[0].wait()
    load_mem.wait()
    own_half(0, k_half)
    pl.semaphore_wait(barrier, 16 + 4 + 1 + 3 + 1 + 2 + 1)

    def first_copy(j):
        t = 2 * lax.rem(j + lax.div(over, 2), 16) + (1 - m)
        return remote(
            feat.at[:, :, pl.ds(pl.multiple_of(t * 128, 128), 128)],
            gath.at[lax.div(k, 2)],
            sent.at[0],
            g_recv.at[0],
            dev(lax.rem(2 * t + 32, 64) + odd, f, lax.rem(k, 2)),
        )

    def send_first(j, _):
        first_copy(j).start()
        return 0

    load_feat.wait()
    lax.fori_loop(0, 16, send_first, 0)

    def part_of(ref, u, at, count=64):
        return ref.at[u, pl.ds(pl.multiple_of(at, 32), count), :]

    def direct(c, parity):
        return lax.rem(c + 8, 4) * 128 + parity * 64

    def around(step):
        return lax.rem(z + 8 + step, 8) * 64

    zp = lax.rem(z, 2)

    def mine_of(u, c):
        if KIND[u] == 0:
            return part_of(got, u, direct(c, 0), 128)
        return part_of(got, u, direct(c, zp) if KIND[u] == 1 else around(0))

    def cross_copy(u):
        if KIND[u] == 0:
            at, count = direct(color + 2, 0), 128
        else:
            at, count = direct(color + 2, zp) if KIND[u] == 1 else around(0), 64
        return remote(
            part_of(own, u, at, count),
            part_of(got, u, at, count),
            sent.at[3 + u],
            c_recv.at[u],
            cross_dev,
        )

    def swap_copy(u):
        ref = part_of(got, u, direct(color, zp))
        return remote(ref, ref, sent.at[3 + u], s_recv.at[KIND[:u].count(1)], z_pair)

    def forward_copy(u, i, late):
        ref = part_of(got, u, direct(color, 1 - zp)) if late else mine_of(u, color)
        return remote(ref, ref, sent.at[3 + u], f_recv.at[u], ring[i])

    def ring_place(u, hop, way, half):
        at = around(hop * (2 * way - 1))
        return part_of(got, u, at + 32 * way, 32) if half else part_of(got, u, at)

    def ring_copy(u, step, way):
        ref = ring_place(u, step, way, step == 3)
        return remote(ref, ref, sent.at[3 + u], z_recv.at[KIND[:u].count(2), step], (z_up, z_down)[way])

    def arrived(ref, sem):
        pltpu.make_async_copy(ref, ref, sem).wait()

    def forward(u):
        arrived(mine_of(u, color), c_recv.at[u])
        if KIND[u] == 1:
            swap_copy(u).start()
        for i in range(3):
            forward_copy(u, i, False).start()

    def second(u):
        arrived(part_of(got, u, direct(color, 1 - zp)), s_recv.at[KIND[:u].count(1)])
        for i in range(3):
            forward_copy(u, i, True).start()

    def ring_arrived(u, step):
        arrived(part_of(got, u, 0, 64 if step == 3 else 128), z_recv.at[KIND[:u].count(2), step])

    def circulate(u, step):
        if step > 0:
            ring_arrived(u, step - 1)
        else:
            arrived(mine_of(u, color), c_recv.at[u])
        for way in range(2):
            ring_copy(u, step, way).start()

    def ready(u):
        if KIND[u] == 2:
            ring_arrived(u, 3)
        else:
            arrived(part_of(got, u, 0, 384), f_recv.at[u])

    def across(units):
        for u in units:
            if u > 0:
                loads[u].wait()
            cross_copy(u).start()

    across(ORDER[:EARLY])

    def second_copy(e):
        rr, to = quad(e)
        return remote(blocks.at[rr], held.at[m, r], sent.at[1], h_recv.at[0], to)

    def relay_copy():
        return remote(held.at[m], held.at[m], sent.at[2], h_recv.at[1], sibling)

    def relay():
        arrived(held.at[m], h_recv.at[0])
        relay_copy().start()

    def send_second(e, _):
        second_copy(e).start()
        return 0

    def turn():
        arrived(gath, g_recv.at[0])
        for fr in range(FRAMES):
            turned = gath[:, fr].astype(F32).reshape(128, 128).T.astype(BF16)
            blocks[:, fr] = turned.reshape(4, STR, 128)
        lax.fori_loop(0, 4, send_second, 0)
        across(ORDER[EARLY:])

    def split_norm(values_f32, chunk):
        at = pl.ds(pl.multiple_of(chunk * 32, 32), 32)
        b = values_f32.astype(BF16)
        n[0, at, :] = b[:, :512]
        n[1, at, :] = b[:, 512:]

    def first_norm(c, _):
        at = pl.ds(pl.multiple_of(c * 32, 32), 32)
        v = normalized(x[at, :]).astype(BF16).astype(F32).reshape(4, ROWS, 1024)
        row = lax.broadcasted_iota(jnp.int32, v.shape, 1)
        summary = jnp.sum(jnp.where(row < GROUP, v, 0.0), axis=1, keepdims=True) * (1.0 / GROUP)
        v = jnp.where(row == FRAMES, summary, v)
        split_norm(v.reshape(32, 1024), c)
        return 0

    def norm():
        arrived(held.at[1 - m], h_recv.at[1])
        for s in range(8):
            xp[:, pl.ds(128 * s, 128)] = held[s // 4, s % 4].reshape(STR * FRAMES, 128)
        for h in range(2):
            half = pl.ds(512 * h, 512)
            placed = dot(xp[...], perm[:, half]).astype(BF16)
            x[:, half] = dot(rows[...], placed)
        lax.fori_loop(0, 8, first_norm, 0, unroll=4)

    ready_once = set()

    def need(u):
        if u not in ready_once:
            ready_once.add(u)
            ready(u)

    def other_half(u, half, place):
        need(u)

        def memory_rows(c, _):
            at = pl.ds(pl.multiple_of(c * 256, 256), 256)
            sums = half[at, :] + dot(memory[at, theirs], got[u])
            place[pl.ds(c * 8, 8), pl.ds(0, MEM), :] = sums.astype(BF16).reshape(8, MEM, 512)
            return 0

        lax.fori_loop(0, 4, memory_rows, 0)

    def group(u, place, center):
        need(u)

        g = (dot(n[f], own[u]) + dot(n[1 - f], got[u])).reshape(STR, ROWS, 512)
        both = jnp.concatenate([g, jnp.zeros_like(g)], axis=1).astype(BF16)
        place[:, pl.ds(MEM + LEFT, 16), :] = both
        center[...] = g[:, :GROUP, :].astype(BF16)

    def query():
        need(2)
        q[...] = (
            (dot(n[f], own[2]) + dot(n[1 - f], got[2])).astype(BF16).astype(F32) * (HD**-0.5)
        ).reshape(STR, ROWS, 512)

    heads = ROWS
    head_mask = jnp.where(
        (lax.broadcasted_iota(jnp.int32, (heads, 512), 1) >> 6)
        == lax.broadcasted_iota(jnp.int32, (heads, 512), 0),
        1.0,
        0.0,
    )
    queries = FRAMES + 1

    width = 4

    def attend(first):
        streams = [first + i for i in range(width)]
        probs = []
        scored = []
        for s in streams:
            q8 = q[s]
            spread = jnp.concatenate(
                [
                    jnp.broadcast_to(q8[i : i + 1], (heads, 512)) * head_mask
                    for i in range(queries)
                ],
                axis=0,
            ).astype(BF16)
            scored.append(
                lax.dot_general(
                    spread, keys[s], (((1,), (1,)), ((), ())), preferred_element_type=F32
                )
            )
        row = lax.broadcasted_iota(jnp.int32, (queries * heads, KEYS), 0)
        col = lax.broadcasted_iota(jnp.int32, (queries * heads, KEYS), 1)
        in_mem = (col < MEM) & (row < FRAMES * heads)
        in_rest = col < MEM + LEFT + FRAMES
        for s, scores in zip(streams, scored):
            seen_mem = (col >= MEM - fill[s]) & in_mem
            seen_left = (col >= MEM + LEFT - length[s]) & in_rest
            scores = jnp.where(seen_mem | seen_left, scores, MASKED)
            e = jnp.exp(scores - jnp.max(scores, axis=-1, keepdims=True))
            probs.append((e / jnp.sum(e, axis=-1, keepdims=True)).astype(BF16))
        for s, p in zip(streams, probs):
            mixed = dot(p, values[s]).reshape(queries, heads, 512)
            att[s, pl.ds(0, queries), :] = jnp.sum(mixed * head_mask[None], axis=1)

    def attend_block(b):
        def few(i, _):
            attend(b * 8 + width * i)
            return 0

        lax.fori_loop(0, 8 // width, few, 0)

    def exchange(src, dst, i):
        return remote(src, dst, e_send.at[i], e_recv.at[i], sibling)

    def output():
        need(3)
        a = att[...].reshape(STR * ROWS, 512).astype(BF16)
        for i, (h, w) in enumerate(((f, own), (1 - f, got))):
            part[h] = dot(a, w[3]).astype(BF16)
            exchange(part.at[h], part_in.at[h], i).start()

    def second_norm(c, _):
        at = pl.ds(pl.multiple_of(c * 32, 32), 32)
        summed = [part[h, at, :].astype(F32) + part_in[h, at, :].astype(F32) for h in range(2)]
        v = x[at, :] + jnp.concatenate(summed, axis=1)
        x[at, :] = v
        split_norm(normalized(v), c)
        return 0

    def norm_two():
        for i, h in enumerate((f, 1 - f)):
            exchange(part.at[h], part_in.at[h], i).wait()
        lax.fori_loop(0, 8, second_norm, 0, unroll=4)

    def next_memory():
        mem_vm[...] = jnp.tanh(x[...].reshape(STR, ROWS, 1024)[:, FRAMES, :]).astype(BF16)
        write[1].start()

    hidden = {}

    def hidden_block(j):
        need(4 + 2 * j)
        sums = dot(n[f], own[4 + 2 * j]) + dot(n[1 - f], got[4 + 2 * j])
        hidden[j] = jax.nn.gelu(sums, approximate=True).astype(BF16)

    def down_block(j):
        need(5 + 2 * j)
        for i, (h, w) in enumerate(((f, own), (1 - f, got))):
            sums = dot(hidden[j], w[5 + 2 * j])
            if j != BLOCKS[0]:
                sums = down[h] + sums
            if j != BLOCKS[3]:
                down[h] = sums
                continue
            down_out[h] = sums.astype(BF16)
            exchange(down_out.at[h], down_in.at[h], 2 + i).start()

    def third_norm(c, _):
        at = pl.ds(pl.multiple_of(c * 32, 32), 32)
        summed = [down_out[h, at, :].astype(F32) + down_in[h, at, :].astype(F32) for h in range(2)]
        v = x[at, :] + jnp.concatenate(summed, axis=1)
        split_norm(normalized(v) * gain[...], c)
        return 0

    def finish():
        for i, h in enumerate((f, 1 - f)):
            exchange(down_out.at[h], down_in.at[h], 2 + i).wait()
        lax.fori_loop(0, 8, third_norm, 0, unroll=4)
        for h in range(2):
            placed = dot(frames_first[...], n[h]).astype(BF16)
            out_vm[:, :, pl.ds(512 * h, 512)] = placed.reshape(FRAMES, STR, 512)
        write[0].start()

    def keys_done():
        load_lk.wait()
        other_half(0, k_half, keys)

    def values_done():
        load_lv.wait()
        other_half(1, v_half, values)

    def group_k():
        group(0, keys, ck_vm)
        write[2].start()

    def group_v():
        group(1, values, cv_vm)
        write[3].start()

    steps = {
        "own_v": lambda: own_half(1, v_half),
        "turn": turn,
        "norm": norm,
        "relay": relay,
        "mem_k": keys_done,
        "mem_v": values_done,
        "group_k": group_k,
        "group_v": group_v,
        "query": query,
        "output": output,
        "norm_two": norm_two,
        "next": next_memory,
        "finish": finish,
    }
    more = {
        "forward": forward,
        "second": second,
        "circulate": circulate,
        "attend": attend_block,
        "hidden": hidden_block,
        "down": down_block,
    }
    for name, *given in STEPS:
        if name in steps:
            steps[name]()
        else:
            more[name](*given)

    arrived(gath, sent.at[0])
    arrived(held.at[m], sent.at[1])
    arrived(held.at[m], sent.at[2])
    for u in range(UNITS):
        arrived(got.at[u], sent.at[3 + u])
    for copy in write:
        copy.wait()


def hand_over(*refs):
    given, held, results, into, out_of = refs[:4], refs[4:8], refs[8:12], refs[12], refs[13]
    arrive = [
        pltpu.make_async_copy(*pair, into.at[i]) for i, pair in enumerate(zip(given, results))
    ]
    leave = [
        pltpu.make_async_copy(*pair, out_of.at[i]) for i, pair in enumerate(zip(results, held))
    ]
    for copy in arrive:
        copy.start()
    for i in range(4):
        arrive[i].wait()
        leave[i].start()
    for copy in leave:
        copy.wait()


def shards(
    features,
    memory_bank,
    memory_fill,
    left_keys,
    left_values,
    left_length,
    w_query,
    w_key,
    w_value,
    w_out,
    w_up,
    w_down,
    out_gain,
):
    memory = memory_bank.reshape(STR * MEM, 1024)
    smem = pl.BlockSpec(memory_space=pltpu.SMEM)
    hbm = pl.BlockSpec(memory_space=pltpu.HBM)
    vmem = pl.BlockSpec(memory_space=pltpu.VMEM)
    dma = pltpu.SemaphoreType.DMA
    shapes = (
        jax.ShapeDtypeStruct((FRAMES, STR, 1024), BF16),
        jax.ShapeDtypeStruct((STR, 1024), BF16),
        jax.ShapeDtypeStruct((STR, GROUP, 512), BF16),
        jax.ShapeDtypeStruct((STR, GROUP, 512), BF16),
    )
    results = pl.pallas_call(
        kernel,
        name="layer",
        out_shape=shapes,
        in_specs=[smem] * 2 + [hbm] * 10 + [vmem],
        out_specs=(hbm,) * 4,
        scratch_shapes=[
            pltpu.VMEM((FRAMES, 8, 4096), BF16),
            pltpu.VMEM((16, FRAMES, 8, 128), BF16),
            pltpu.VMEM((4, FRAMES, STR, 128), BF16),
            pltpu.VMEM((2, 4, FRAMES, STR, 128), BF16),
            pltpu.VMEM((1024, 1024), BF16),
            pltpu.VMEM((STR * ROWS, STR * FRAMES), BF16),
            pltpu.VMEM((STR * FRAMES, STR * ROWS), BF16),
            pltpu.VMEM((STR * FRAMES, 1024), BF16),
            pltpu.VMEM((STR * ROWS, 1024), F32),
            pltpu.VMEM((2, STR * ROWS, 512), BF16),
            pltpu.VMEM((UNITS, 512, 512), BF16),
            pltpu.VMEM((UNITS, 512, 512), BF16),
            pltpu.VMEM((STR * MEM, 1024), BF16),
            pltpu.VMEM((STR, KEYS, 512), BF16),
            pltpu.VMEM((STR, KEYS, 512), BF16),
            pltpu.VMEM((STR, ROWS, 512), F32),
            pltpu.VMEM((STR, ROWS, 512), F32),
            pltpu.VMEM((2, STR * ROWS, 512), BF16),
            pltpu.VMEM((2, STR * ROWS, 512), BF16),
            pltpu.VMEM((2, STR * ROWS, 512), F32),
            pltpu.VMEM((2, STR * ROWS, 512), BF16),
            pltpu.VMEM((2, STR * ROWS, 512), BF16),
            pltpu.VMEM((STR * MEM, 512), F32),
            pltpu.VMEM((STR * MEM, 512), F32),
            *[pltpu.VMEM(v.shape, v.dtype) for v in shapes],
            dma((4,)),
            dma((UNITS + 4,)),
            dma((3 + UNITS,)),
            dma((1,)),
            dma((2,)),
            dma((UNITS,)),
            dma((max(1, KIND.count(1)),)),
            dma((UNITS,)),
            dma((max(1, KIND.count(2)), 4)),
            dma((4,)),
            dma((4,)),
        ],
        compiler_params=pltpu.CompilerParams(
            collective_id=0, has_side_effects=True, vmem_limit_bytes=62_600_000
        ),
    )(
        memory_fill,
        left_length,
        features,
        memory,
        left_keys,
        left_values,
        w_query,
        w_key,
        w_value,
        w_out,
        w_up,
        w_down,
        out_gain.reshape(1, 1024),
    )
    layer_out, memory_next, center_keys, center_values = pl.pallas_call(
        hand_over,
        name="hand_over",
        out_shape=shapes,
        in_specs=[hbm] * 4,
        out_specs=(hbm,) * 4,
        scratch_shapes=[pltpu.VMEM(v.shape, v.dtype) for v in shapes] + [dma((4,)), dma((4,))],
        compiler_params=pltpu.CompilerParams(vmem_limit_bytes=62_600_000),
    )(*results)
    return jnp.transpose(layer_out, (1, 0, 2)), memory_next, center_keys, center_values


def solution(mesh):
    in_specs = (
        P(None, ("dp", "fsdp"), None),
        P(("dp", "fsdp"), None, None),
        P(("dp", "fsdp")),
        P(("dp", "fsdp"), None, "mp"),
        P(("dp", "fsdp"), None, "mp"),
        P(("dp", "fsdp")),
        P("fsdp", "mp"),
        P("fsdp", "mp"),
        P("fsdp", "mp"),
        P("mp", "fsdp"),
        P("fsdp", "mp"),
        P("mp", "fsdp"),
        P(),
    )
    out_specs = (
        P(("dp", "fsdp"), None, None),
        P(("dp", "fsdp"), None),
        P(("dp", "fsdp"), None, "mp"),
        P(("dp", "fsdp"), None, "mp"),
    )
    return jax.shard_map(shards, mesh=mesh, in_specs=in_specs, out_specs=out_specs, check_vma=False)
```

```python
import functools

import jax
import jax.numpy as jnp
from jax import lax
from jax.experimental import pallas as pl
from jax.experimental.pallas import tpu as pltpu
from jax.sharding import PartitionSpec as P

HD = 64
GROUP = 4
FRAMES = 5
MEM = 32
LEFT = 64
STR = 32
ROWS = 8
KEYS = 112
UNITS = 12
KIND = (1, 1, 1, 0, 2, 0, 2, 0, 0, 1, 2, 0)
ORDER = (1, 2, 0, 4, 10, 6, 9, 3, 11, 5, 8, 7)
EARLY = 4
BLOCKS = (0, 2, 3, 1)
STEPS = (
    ("own_v", 0),
    ("forward", 1),
    ("turn", 0),
    ("forward", 2),
    ("forward", 0),
    ("second", 1),
    ("circulate", 4, 0),
    ("relay", 0),
    ("second", 2),
    ("circulate", 10, 0),
    ("norm", 0),
    ("second", 0),
    ("circulate", 6, 0),
    ("mem_v", 0),
    ("forward", 9),
    ("circulate", 4, 1),
    ("group_v", 0),
    ("query", 0),
    ("circulate", 10, 1),
    ("forward", 3),
    ("mem_k", 0),
    ("group_k", 0),
    ("circulate", 6, 1),
    ("second", 9),
    ("attend", 0),
    ("forward", 11),
    ("attend", 1),
    ("circulate", 4, 2),
    ("attend", 2),
    ("forward", 5),
    ("circulate", 10, 2),
    ("attend", 3),
    ("output", 0),
    ("circulate", 6, 2),
    ("forward", 8),
    ("norm_two", 0),
    ("next", 0),
    ("circulate", 4, 3),
    ("circulate", 10, 3),
    ("forward", 7),
    ("circulate", 6, 3),
    ("hidden", 0),
    ("down", 0),
    ("hidden", 2),
    ("down", 2),
    ("hidden", 3),
    ("down", 3),
    ("hidden", 1),
    ("down", 1),
    ("finish", 0),
)
EPS = 1e-05
MASKED = -1e30
F32 = jnp.float32
BF16 = jnp.bfloat16


def dot(a, b):
    return jnp.dot(a, b, preferred_element_type=F32)


def normalized(x):
    mean = jnp.sum(x, axis=-1, keepdims=True) * (1.0 / x.shape[-1])
    cent = x - mean
    var = jnp.sum(cent * cent, axis=-1, keepdims=True) * (1.0 / x.shape[-1])
    return cent * lax.rsqrt(var + EPS)


def kernel(
    fill_hbm,
    length_hbm,
    feat_hbm,
    mem_hbm,
    lk_hbm,
    lv_hbm,
    wq_hbm,
    wk_hbm,
    wv_hbm,
    wo_hbm,
    wu_hbm,
    wd_hbm,
    gain_hbm,
    out,
    mem_next,
    center_k,
    center_v,
    feat,
    gath,
    blocks,
    held,
    perm,
    rows,
    frames_first,
    xp,
    x,
    n,
    own,
    got,
    memory,
    keys,
    values,
    q,
    att,
    part,
    part_in,
    down,
    down_out,
    down_in,
    k_half,
    v_half,
    out_vm,
    mem_vm,
    ck_vm,
    cv_vm,
    fill,
    length,
    gain,
    o_sem,
    l_sem,
    sent,
    g_recv,
    h_recv,
    c_recv,
    s_recv,
    f_recv,
    z_recv,
    e_send,
    e_recv,
):
    d = lax.axis_index("dp")
    m = lax.axis_index("mp")
    f = lax.axis_index("fsdp")
    xl = lax.div(d, 32)
    y = lax.rem(lax.div(d, 8), 4)
    z = lax.rem(d, 8)
    k = lax.div(d, 2)
    odd = lax.rem(d, 2)
    r = odd * 2 + f
    color = lax.rem(y + 2 * xl, 4)

    def dev(dd, ff, mm):
        return {"dp": dd, "fsdp": ff, "mp": mm}

    def remote(src, dst, send, recv, to):
        return pltpu.make_async_remote_copy(
            src_ref=src,
            dst_ref=dst,
            send_sem=send,
            recv_sem=recv,
            device_id=to,
            device_id_type=pl.DeviceIdType.MESH,
        )

    flipped = d + 32 * (1 - 2 * xl)
    over = lax.div(flipped, 2)
    z_up = dev(d - z + lax.rem(z + 1, 8), f, m)
    z_down = dev(d - z + lax.rem(z + 7, 8), f, m)
    z_pair = dev(d + 1 - 2 * odd, f, m)
    up_d = xl * 32 + lax.rem(y + 1, 4) * 8 + z
    down_d = xl * 32 + lax.rem(y + 3, 4) * 8 + z
    cross_dev = dev(flipped, 1 - f, m)
    ring = (dev(flipped, f, m), dev(up_d, f, m), dev(down_d, f, m))
    sibling = dev(d, f, 1 - m)

    write = [
        pltpu.make_async_copy(src, dst, o_sem.at[i])
        for i, (src, dst) in enumerate(
            ((out_vm, out), (mem_vm, mem_next), (ck_vm, center_k), (cv_vm, center_v))
        )
    ]

    def load(i, src, dst):
        return pltpu.make_async_copy(src, dst, l_sem.at[i])

    units = [wk_hbm, wv_hbm, wq_hbm, wo_hbm]
    for j in range(4):
        units.append(wu_hbm.at[:, pl.ds(512 * j, 512)])
        units.append(wd_hbm.at[pl.ds(512 * j, 512), :])
    loads = [load(u, units[u], own.at[u]) for u in range(UNITS)]
    load_feat = load(UNITS, feat_hbm, feat)
    load_mem = load(UNITS + 1, mem_hbm, memory)
    load_lk = load(UNITS + 2, lk_hbm, keys.at[:, pl.ds(MEM, LEFT), :])
    load_lv = load(UNITS + 3, lv_hbm, values.at[:, pl.ds(MEM, LEFT), :])
    small = [
        load(UNITS + 4, fill_hbm, fill),
        load(UNITS + 5, length_hbm, length),
        load(UNITS + 6, gain_hbm, gain),
    ]
    barrier = pltpu.get_barrier_semaphore()

    def greet(to):
        pl.semaphore_signal(
            barrier, inc=1, device_id=to, device_id_type=pl.DeviceIdType.MESH
        )

    def greet_sources(j, _):
        kk = 2 * j + m
        greet(dev(2 * kk + odd, f, 1 - lax.rem(k, 2)))
        return 0

    lax.fori_loop(0, 16, greet_sources, 0)

    def quad(e):
        rr = lax.rem(r + e, 4)
        return rr, dev(2 * over + lax.div(rr, 2), lax.rem(rr, 2), m)

    def greet_quad(e, _):
        greet(quad(e)[1])
        return 0

    lax.fori_loop(0, 4, greet_quad, 0)
    greet(cross_dev)
    for to in ring:
        greet(to)
    greet(sibling)
    greet(z_up)
    greet(z_down)
    greet(z_pair)

    load_feat.start()
    loads[0].start()
    load_mem.start()
    for u in ORDER:
        if u > 0:
            loads[u].start()
    load_lk.start()
    load_lv.start()
    for c in small:
        c.start()

    def build_perm(s, _):
        at = lax.broadcasted_iota(jnp.int32, (128, 1024), 0)
        col = lax.broadcasted_iota(jnp.int32, (128, 1024), 1)
        want = (at >> 3) * 64 + lax.div(s, 4) * 32 + lax.rem(s, 4) * 8 + (at & 7)
        perm[pl.ds(pl.multiple_of(s * 128, 128), 128), :] = jnp.where(
            col == want, 1.0, 0.0
        ).astype(BF16)
        return 0

    lax.fori_loop(0, 8, build_perm, 0)
    at = lax.broadcasted_iota(jnp.int32, (STR * ROWS, STR * FRAMES), 0)
    col = lax.broadcasted_iota(jnp.int32, (STR * ROWS, STR * FRAMES), 1)
    rows[...] = jnp.where(col == (at & 7) * STR + (at >> 3), 1.0, 0.0).astype(BF16)
    at = lax.broadcasted_iota(jnp.int32, (STR * FRAMES, STR * ROWS), 0)
    col = lax.broadcasted_iota(jnp.int32, (STR * FRAMES, STR * ROWS), 1)
    frames_first[...] = jnp.where(col == (at & 31) * ROWS + (at >> 5), 1.0, 0.0).astype(BF16)
    att[...] = jnp.zeros_like(att)

    mine = pl.ds(pl.multiple_of(f * 512, 512), 512)
    theirs = pl.ds(pl.multiple_of((1 - f) * 512, 512), 512)

    def own_half(u, place):
        def memory_rows(c, _):
            at = pl.ds(pl.multiple_of(c * 256, 256), 256)
            place[at, :] = dot(memory[at, mine], own[u])
            return 0

        lax.fori_loop(0, 4, memory_rows, 0)

    loads[0].wait()
    load_mem.wait()
    own_half(0, k_half)
    pl.semaphore_wait(barrier, 16 + 4 + 1 + 3 + 1 + 2 + 1)

    def first_copy(j):
        t = 2 * lax.rem(j + lax.div(over, 2), 16) + (1 - m)
        return remote(
            feat.at[:, :, pl.ds(pl.multiple_of(t * 128, 128), 128)],
            gath.at[lax.div(k, 2)],
            sent.at[0],
            g_recv.at[0],
            dev(lax.rem(2 * t + 32, 64) + odd, f, lax.rem(k, 2)),
        )

    def send_first(j, _):
        first_copy(j).start()
        return 0

    load_feat.wait()
    lax.fori_loop(0, 16, send_first, 0)

    def part_of(ref, u, at, count=64):
        return ref.at[u, pl.ds(pl.multiple_of(at, 32), count), :]

    def direct(c, parity):
        return lax.rem(c + 8, 4) * 128 + parity * 64

    def around(step):
        return lax.rem(z + 8 + step, 8) * 64

    zp = lax.rem(z, 2)

    def mine_of(u, c):
        if KIND[u] == 0:
            return part_of(got, u, direct(c, 0), 128)
        return part_of(got, u, direct(c, zp) if KIND[u] == 1 else around(0))

    def cross_copy(u):
        if KIND[u] == 0:
            at, count = direct(color + 2, 0), 128
        else:
            at, count = direct(color + 2, zp) if KIND[u] == 1 else around(0), 64
        return remote(
            part_of(own, u, at, count),
            part_of(got, u, at, count),
            sent.at[3 + u],
            c_recv.at[u],
            cross_dev,
        )

    def swap_copy(u):
        ref = part_of(got, u, direct(color, zp))
        return remote(ref, ref, sent.at[3 + u], s_recv.at[KIND[:u].count(1)], z_pair)

    def forward_copy(u, i, late):
        ref = part_of(got, u, direct(color, 1 - zp)) if late else mine_of(u, color)
        return remote(ref, ref, sent.at[3 + u], f_recv.at[u], ring[i])

    def ring_place(u, hop, way, half):
        at = around(hop * (2 * way - 1))
        return part_of(got, u, at + 32 * way, 32) if half else part_of(got, u, at)

    def ring_copy(u, step, way):
        ref = ring_place(u, step, way, step == 3)
        return remote(ref, ref, sent.at[3 + u], z_recv.at[KIND[:u].count(2), step], (z_up, z_down)[way])

    def arrived(ref, sem):
        pltpu.make_async_copy(ref, ref, sem).wait()

    def forward(u):
        arrived(mine_of(u, color), c_recv.at[u])
        if KIND[u] == 1:
            swap_copy(u).start()
        for i in range(3):
            forward_copy(u, i, False).start()

    def second(u):
        arrived(part_of(got, u, direct(color, 1 - zp)), s_recv.at[KIND[:u].count(1)])
        for i in range(3):
            forward_copy(u, i, True).start()

    def ring_arrived(u, step):
        arrived(part_of(got, u, 0, 64 if step == 3 else 128), z_recv.at[KIND[:u].count(2), step])

    def circulate(u, step):
        if step > 0:
            ring_arrived(u, step - 1)
        else:
            arrived(mine_of(u, color), c_recv.at[u])
        for way in range(2):
            ring_copy(u, step, way).start()

    def ready(u):
        if KIND[u] == 2:
            ring_arrived(u, 3)
        else:
            arrived(part_of(got, u, 0, 384), f_recv.at[u])

    def across(units):
        for u in units:
            if u > 0:
                loads[u].wait()
            cross_copy(u).start()

    across(ORDER[:EARLY])

    def second_copy(e):
        rr, to = quad(e)
        return remote(blocks.at[rr], held.at[m, r], sent.at[1], h_recv.at[0], to)

    def relay_copy():
        return remote(held.at[m], held.at[m], sent.at[2], h_recv.at[1], sibling)

    def relay():
        arrived(held.at[m], h_recv.at[0])
        relay_copy().start()

    def send_second(e, _):
        second_copy(e).start()
        return 0

    def turn():
        arrived(gath, g_recv.at[0])
        for fr in range(FRAMES):
            turned = gath[:, fr].astype(F32).reshape(128, 128).T.astype(BF16)
            blocks[:, fr] = turned.reshape(4, STR, 128)
        lax.fori_loop(0, 4, send_second, 0)
        across(ORDER[EARLY:])

    def split_norm(values_f32, chunk):
        at = pl.ds(pl.multiple_of(chunk * 32, 32), 32)
        b = values_f32.astype(BF16)
        n[0, at, :] = b[:, :512]
        n[1, at, :] = b[:, 512:]

    def first_norm(c, _):
        at = pl.ds(pl.multiple_of(c * 32, 32), 32)
        v = normalized(x[at, :]).astype(BF16).astype(F32).reshape(4, ROWS, 1024)
        row = lax.broadcasted_iota(jnp.int32, v.shape, 1)
        summary = jnp.sum(jnp.where(row < GROUP, v, 0.0), axis=1, keepdims=True) * (1.0 / GROUP)
        v = jnp.where(row == FRAMES, summary, v)
        split_norm(v.reshape(32, 1024), c)
        return 0

    def norm():
        arrived(held.at[1 - m], h_recv.at[1])
        for s in range(8):
            xp[:, pl.ds(128 * s, 128)] = held[s // 4, s % 4].reshape(STR * FRAMES, 128)
        for h in range(2):
            half = pl.ds(512 * h, 512)
            placed = dot(xp[...], perm[:, half]).astype(BF16)
            x[:, half] = dot(rows[...], placed)
        lax.fori_loop(0, 8, first_norm, 0, unroll=4)

    ready_once = set()

    def need(u):
        if u not in ready_once:
            ready_once.add(u)
            ready(u)

    def other_half(u, half, place):
        need(u)

        def memory_rows(c, _):
            at = pl.ds(pl.multiple_of(c * 256, 256), 256)
            sums = half[at, :] + dot(memory[at, theirs], got[u])
            place[pl.ds(c * 8, 8), pl.ds(0, MEM), :] = sums.astype(BF16).reshape(8, MEM, 512)
            return 0

        lax.fori_loop(0, 4, memory_rows, 0)

    def group(u, place, center):
        need(u)

        g = (dot(n[f], own[u]) + dot(n[1 - f], got[u])).reshape(STR, ROWS, 512)
        both = jnp.concatenate([g, jnp.zeros_like(g)], axis=1).astype(BF16)
        place[:, pl.ds(MEM + LEFT, 16), :] = both
        center[...] = g[:, :GROUP, :].astype(BF16)

    def query():
        need(2)
        q[...] = (
            (dot(n[f], own[2]) + dot(n[1 - f], got[2])).astype(BF16).astype(F32) * (HD**-0.5)
        ).reshape(STR, ROWS, 512)

    heads = ROWS
    head_mask = jnp.where(
        (lax.broadcasted_iota(jnp.int32, (heads, 512), 1) >> 6)
        == lax.broadcasted_iota(jnp.int32, (heads, 512), 0),
        1.0,
        0.0,
    )
    queries = FRAMES + 1

    width = 8

    def attend(first):
        streams = [first + i for i in range(width)]
        probs = []
        scored = []
        for s in streams:
            q8 = q[s]
            spread = jnp.concatenate(
                [
                    jnp.broadcast_to(q8[i : i + 1], (heads, 512)) * head_mask
                    for i in range(queries)
                ],
                axis=0,
            ).astype(BF16)
            scored.append(
                lax.dot_general(
                    spread, keys[s], (((1,), (1,)), ((), ())), preferred_element_type=F32
                )
            )
        row = lax.broadcasted_iota(jnp.int32, (queries * heads, KEYS), 0)
        col = lax.broadcasted_iota(jnp.int32, (queries * heads, KEYS), 1)
        in_mem = (col < MEM) & (row < FRAMES * heads)
        in_rest = col < MEM + LEFT + FRAMES
        for s, scores in zip(streams, scored):
            seen_mem = (col >= MEM - fill[s]) & in_mem
            seen_left = (col >= MEM + LEFT - length[s]) & in_rest
            scores = jnp.where(seen_mem | seen_left, scores, MASKED)
            e = jnp.exp(scores - jnp.max(scores, axis=-1, keepdims=True))
            probs.append((e / jnp.sum(e, axis=-1, keepdims=True)).astype(BF16))
        for s, p in zip(streams, probs):
            mixed = dot(p, values[s]).reshape(queries, heads, 512)
            att[s, pl.ds(0, queries), :] = jnp.sum(mixed * head_mask[None], axis=1)

    def attend_block(b):
        def few(i, _):
            attend(b * 8 + width * i)
            return 0

        lax.fori_loop(0, 8 // width, few, 0)

    def exchange(src, dst, i):
        return remote(src, dst, e_send.at[i], e_recv.at[i], sibling)

    def output():
        need(3)
        a = att[...].reshape(STR * ROWS, 512).astype(BF16)
        for i, (h, w) in enumerate(((f, own), (1 - f, got))):
            part[h] = dot(a, w[3]).astype(BF16)
            exchange(part.at[h], part_in.at[h], i).start()

    def second_norm(c, _):
        at = pl.ds(pl.multiple_of(c * 32, 32), 32)
        summed = [part[h, at, :].astype(F32) + part_in[h, at, :].astype(F32) for h in range(2)]
        v = x[at, :] + jnp.concatenate(summed, axis=1)
        x[at, :] = v
        split_norm(normalized(v), c)
        return 0

    def norm_two():
        for i, h in enumerate((f, 1 - f)):
            exchange(part.at[h], part_in.at[h], i).wait()
        lax.fori_loop(0, 8, second_norm, 0, unroll=4)

    def next_memory():
        mem_vm[...] = jnp.tanh(x[...].reshape(STR, ROWS, 1024)[:, FRAMES, :]).astype(BF16)
        write[1].start()

    hidden = {}

    def hidden_block(j):
        need(4 + 2 * j)
        sums = dot(n[f], own[4 + 2 * j]) + dot(n[1 - f], got[4 + 2 * j])
        hidden[j] = jax.nn.gelu(sums, approximate=True).astype(BF16)

    def down_block(j):
        need(5 + 2 * j)
        for i, (h, w) in enumerate(((f, own), (1 - f, got))):
            sums = dot(hidden[j], w[5 + 2 * j])
            if j != BLOCKS[0]:
                sums = down[h] + sums
            if j != BLOCKS[3]:
                down[h] = sums
                continue
            down_out[h] = sums.astype(BF16)
            exchange(down_out.at[h], down_in.at[h], 2 + i).start()

    def third_norm(c, _):
        at = pl.ds(pl.multiple_of(c * 32, 32), 32)
        summed = [down_out[h, at, :].astype(F32) + down_in[h, at, :].astype(F32) for h in range(2)]
        v = x[at, :] + jnp.concatenate(summed, axis=1)
        split_norm(normalized(v) * gain[...], c)
        return 0

    def finish():
        for i, h in enumerate((f, 1 - f)):
            exchange(down_out.at[h], down_in.at[h], 2 + i).wait()
        lax.fori_loop(0, 8, third_norm, 0, unroll=4)
        for h in range(2):
            placed = dot(frames_first[...], n[h]).astype(BF16)
            out_vm[:, :, pl.ds(512 * h, 512)] = placed.reshape(FRAMES, STR, 512)
        write[0].start()

    def keys_done():
        for c in small:
            c.wait()
        load_lk.wait()
        other_half(0, k_half, keys)

    def values_done():
        load_lv.wait()
        other_half(1, v_half, values)

    def group_k():
        group(0, keys, ck_vm)
        write[2].start()

    def group_v():
        group(1, values, cv_vm)
        write[3].start()

    steps = {
        "own_v": lambda: own_half(1, v_half),
        "turn": turn,
        "norm": norm,
        "relay": relay,
        "mem_k": keys_done,
        "mem_v": values_done,
        "group_k": group_k,
        "group_v": group_v,
        "query": query,
        "output": output,
        "norm_two": norm_two,
        "next": next_memory,
        "finish": finish,
    }
    more = {
        "forward": forward,
        "second": second,
        "circulate": circulate,
        "attend": attend_block,
        "hidden": hidden_block,
        "down": down_block,
    }
    for name, *given in STEPS:
        if name in steps:
            steps[name]()
        else:
            more[name](*given)

    arrived(gath, sent.at[0])
    arrived(held.at[m], sent.at[1])
    arrived(held.at[m], sent.at[2])
    for u in range(UNITS):
        arrived(got.at[u], sent.at[3 + u])
    for copy in write:
        copy.wait()


def hand_over(*refs):
    sems = refs[8]
    leave = [pltpu.make_async_copy(refs[i], refs[4 + i], sems.at[i]) for i in range(4)]
    for copy in leave:
        copy.start()
    for copy in leave:
        copy.wait()


def shards(
    features,
    memory_bank,
    memory_fill,
    left_keys,
    left_values,
    left_length,
    w_query,
    w_key,
    w_value,
    w_out,
    w_up,
    w_down,
    out_gain,
):
    memory = memory_bank.reshape(STR * MEM, 1024)
    hbm = pl.BlockSpec(memory_space=pltpu.HBM)
    either = pl.BlockSpec(memory_space=pl.ANY)
    dma = pltpu.SemaphoreType.DMA
    shapes = (
        jax.ShapeDtypeStruct((FRAMES, STR, 1024), BF16),
        jax.ShapeDtypeStruct((STR, 1024), BF16),
        jax.ShapeDtypeStruct((STR, GROUP, 512), BF16),
        jax.ShapeDtypeStruct((STR, GROUP, 512), BF16),
    )
    results = pl.pallas_call(
        kernel,
        name="layer",
        out_shape=shapes,
        in_specs=[hbm] * 13,
        out_specs=(either,) * 4,
        scratch_shapes=[
            pltpu.VMEM((FRAMES, 8, 4096), BF16),
            pltpu.VMEM((16, FRAMES, 8, 128), BF16),
            pltpu.VMEM((4, FRAMES, STR, 128), BF16),
            pltpu.VMEM((2, 4, FRAMES, STR, 128), BF16),
            pltpu.VMEM((1024, 1024), BF16),
            pltpu.VMEM((STR * ROWS, STR * FRAMES), BF16),
            pltpu.VMEM((STR * FRAMES, STR * ROWS), BF16),
            pltpu.VMEM((STR * FRAMES, 1024), BF16),
            pltpu.VMEM((STR * ROWS, 1024), F32),
            pltpu.VMEM((2, STR * ROWS, 512), BF16),
            pltpu.VMEM((UNITS, 512, 512), BF16),
            pltpu.VMEM((UNITS, 512, 512), BF16),
            pltpu.VMEM((STR * MEM, 1024), BF16),
            pltpu.VMEM((STR, KEYS, 512), BF16),
            pltpu.VMEM((STR, KEYS, 512), BF16),
            pltpu.VMEM((STR, ROWS, 512), F32),
            pltpu.VMEM((STR, ROWS, 512), F32),
            pltpu.VMEM((2, STR * ROWS, 512), BF16),
            pltpu.VMEM((2, STR * ROWS, 512), BF16),
            pltpu.VMEM((2, STR * ROWS, 512), F32),
            pltpu.VMEM((2, STR * ROWS, 512), BF16),
            pltpu.VMEM((2, STR * ROWS, 512), BF16),
            pltpu.VMEM((STR * MEM, 512), F32),
            pltpu.VMEM((STR * MEM, 512), F32),
            *[pltpu.VMEM(v.shape, v.dtype) for v in shapes],
            pltpu.SMEM((STR,), jnp.int32),
            pltpu.SMEM((STR,), jnp.int32),
            pltpu.VMEM((1, 1024), F32),
            dma((4,)),
            dma((UNITS + 7,)),
            dma((3 + UNITS,)),
            dma((1,)),
            dma((2,)),
            dma((UNITS,)),
            dma((max(1, KIND.count(1)),)),
            dma((UNITS,)),
            dma((max(1, KIND.count(2)), 4)),
            dma((4,)),
            dma((4,)),
        ],
        compiler_params=pltpu.CompilerParams(
            collective_id=0, has_side_effects=True, vmem_limit_bytes=46_000_000
        ),
    )(
        *[
            pltpu.with_memory_space_constraint(v, pltpu.HBM)
            for v in (
                memory_fill,
                left_length,
                features,
                memory,
                left_keys,
                left_values,
                w_query,
                w_key,
                w_value,
                w_out,
                w_up,
                w_down,
                out_gain.reshape(1, 1024),
            )
        ]
    )
    layer_out, memory_next, center_keys, center_values = pl.pallas_call(
        hand_over,
        name="hand_over",
        out_shape=shapes,
        in_specs=[either] * 4,
        out_specs=(hbm,) * 4,
        scratch_shapes=[dma((4,))],
        compiler_params=pltpu.CompilerParams(vmem_limit_bytes=1_000_000),
    )(*results)
    return jnp.transpose(layer_out, (1, 0, 2)), memory_next, center_keys, center_values


def solution(mesh):
    in_specs = (
        P(None, ("dp", "fsdp"), None),
        P(("dp", "fsdp"), None, None),
        P(("dp", "fsdp")),
        P(("dp", "fsdp"), None, "mp"),
        P(("dp", "fsdp"), None, "mp"),
        P(("dp", "fsdp")),
        P("fsdp", "mp"),
        P("fsdp", "mp"),
        P("fsdp", "mp"),
        P("mp", "fsdp"),
        P("fsdp", "mp"),
        P("mp", "fsdp"),
        P(),
    )
    out_specs = (
        P(("dp", "fsdp"), None, None),
        P(("dp", "fsdp"), None),
        P(("dp", "fsdp"), None, "mp"),
        P(("dp", "fsdp"), None, "mp"),
    )
    return jax.shard_map(shards, mesh=mesh, in_specs=in_specs, out_specs=out_specs, check_vma=False)
```

```python
import functools

import jax
import jax.numpy as jnp
from jax import lax
from jax.experimental import pallas as pl
from jax.experimental.pallas import tpu as pltpu
from jax.sharding import PartitionSpec as P

HD = 64
GROUP = 4
FRAMES = 5
MEM = 32
LEFT = 64
STR = 32
ROWS = 8
KEYS = 112
UNITS = 12
KIND = (1, 1, 1, 0, 2, 0, 2, 0, 0, 1, 2, 0)
ORDER = (1, 2, 0, 4, 10, 6, 9, 3, 11, 5, 8, 7)
EARLY = 4
BLOCKS = (0, 2, 3, 1)
STEPS = (
    ("own_v", 0),
    ("forward", 1),
    ("turn", 0),
    ("forward", 2),
    ("forward", 0),
    ("second", 1),
    ("circulate", 4, 0),
    ("relay", 0),
    ("second", 2),
    ("circulate", 10, 0),
    ("norm", 0),
    ("second", 0),
    ("circulate", 6, 0),
    ("mem_v", 0),
    ("forward", 9),
    ("circulate", 4, 1),
    ("group_v", 0),
    ("query", 0),
    ("circulate", 10, 1),
    ("forward", 3),
    ("mem_k", 0),
    ("group_k", 0),
    ("circulate", 6, 1),
    ("second", 9),
    ("attend", 0),
    ("forward", 11),
    ("attend", 1),
    ("circulate", 4, 2),
    ("attend", 2),
    ("forward", 5),
    ("circulate", 10, 2),
    ("attend", 3),
    ("output", 0),
    ("circulate", 6, 2),
    ("forward", 8),
    ("norm_two", 0),
    ("next", 0),
    ("circulate", 4, 3),
    ("forward", 7),
    ("circulate", 10, 3),
    ("circulate", 6, 3),
    ("hidden", 0),
    ("down", 0),
    ("hidden", 2),
    ("down", 2),
    ("hidden", 3),
    ("down", 3),
    ("hidden", 1),
    ("down", 1),
    ("finish", 0),
)
EPS = 1e-05
MASKED = -1e30
F32 = jnp.float32
BF16 = jnp.bfloat16


def dot(a, b):
    return jnp.dot(a, b, preferred_element_type=F32)


def normalized(x):
    mean = jnp.sum(x, axis=-1, keepdims=True) * (1.0 / x.shape[-1])
    cent = x - mean
    var = jnp.sum(cent * cent, axis=-1, keepdims=True) * (1.0 / x.shape[-1])
    return cent * lax.rsqrt(var + EPS)


def kernel(
    fill_hbm,
    length_hbm,
    feat_hbm,
    mem_hbm,
    lk_hbm,
    lv_hbm,
    wq_hbm,
    wk_hbm,
    wv_hbm,
    wo_hbm,
    wu_hbm,
    wd_hbm,
    gain_hbm,
    out,
    mem_next,
    center_k,
    center_v,
    feat,
    gath,
    blocks,
    held,
    perm,
    rows,
    frames_first,
    xp,
    x,
    n,
    own,
    got,
    memory,
    keys,
    values,
    q,
    att,
    part,
    part_in,
    down,
    down_out,
    down_in,
    k_half,
    v_half,
    out_vm,
    mem_vm,
    ck_vm,
    cv_vm,
    fill,
    length,
    gain,
    o_sem,
    l_sem,
    sent,
    g_recv,
    h_recv,
    c_recv,
    s_recv,
    f_recv,
    z_recv,
    e_send,
    e_recv,
):
    d = lax.axis_index("dp")
    m = lax.axis_index("mp")
    f = lax.axis_index("fsdp")
    xl = lax.div(d, 32)
    y = lax.rem(lax.div(d, 8), 4)
    z = lax.rem(d, 8)
    k = lax.div(d, 2)
    odd = lax.rem(d, 2)
    r = odd * 2 + f
    color = lax.rem(y + 2 * xl, 4)

    def dev(dd, ff, mm):
        return {"dp": dd, "fsdp": ff, "mp": mm}

    def remote(src, dst, send, recv, to):
        return pltpu.make_async_remote_copy(
            src_ref=src,
            dst_ref=dst,
            send_sem=send,
            recv_sem=recv,
            device_id=to,
            device_id_type=pl.DeviceIdType.MESH,
        )

    flipped = d + 32 * (1 - 2 * xl)
    over = lax.div(flipped, 2)
    z_up = dev(d - z + lax.rem(z + 1, 8), f, m)
    z_down = dev(d - z + lax.rem(z + 7, 8), f, m)
    z_pair = dev(d + 1 - 2 * odd, f, m)
    up_d = xl * 32 + lax.rem(y + 1, 4) * 8 + z
    down_d = xl * 32 + lax.rem(y + 3, 4) * 8 + z
    cross_dev = dev(flipped, 1 - f, m)
    ring = (dev(flipped, f, m), dev(up_d, f, m), dev(down_d, f, m))
    sibling = dev(d, f, 1 - m)

    write = [
        pltpu.make_async_copy(src, dst, o_sem.at[i])
        for i, (src, dst) in enumerate(
            ((out_vm, out), (mem_vm, mem_next), (ck_vm, center_k), (cv_vm, center_v))
        )
    ]

    def load(i, src, dst):
        return pltpu.make_async_copy(src, dst, l_sem.at[i])

    units = [wk_hbm, wv_hbm, wq_hbm, wo_hbm]
    for j in range(4):
        units.append(wu_hbm.at[:, pl.ds(512 * j, 512)])
        units.append(wd_hbm.at[pl.ds(512 * j, 512), :])
    loads = [load(u, units[u], own.at[u]) for u in range(UNITS)]
    load_feat = load(UNITS, feat_hbm, feat)
    load_mem = load(UNITS + 1, mem_hbm, memory)
    load_lk = load(UNITS + 2, lk_hbm, keys.at[:, pl.ds(MEM, LEFT), :])
    load_lv = load(UNITS + 3, lv_hbm, values.at[:, pl.ds(MEM, LEFT), :])
    small = [
        load(UNITS + 4, fill_hbm, fill),
        load(UNITS + 5, length_hbm, length),
        load(UNITS + 6, gain_hbm, gain),
    ]
    barrier = pltpu.get_barrier_semaphore()

    def greet(to):
        pl.semaphore_signal(
            barrier, inc=1, device_id=to, device_id_type=pl.DeviceIdType.MESH
        )

    def greet_sources(j, _):
        kk = 2 * j + m
        greet(dev(2 * kk + odd, f, 1 - lax.rem(k, 2)))
        return 0

    lax.fori_loop(0, 16, greet_sources, 0)

    def quad(e):
        rr = lax.rem(r + e, 4)
        return rr, dev(2 * over + lax.div(rr, 2), lax.rem(rr, 2), m)

    def greet_quad(e, _):
        greet(quad(e)[1])
        return 0

    lax.fori_loop(0, 4, greet_quad, 0)
    greet(cross_dev)
    for to in ring:
        greet(to)
    greet(sibling)
    greet(z_up)
    greet(z_down)
    greet(z_pair)

    load_feat.start()
    loads[0].start()
    load_mem.start()
    for u in ORDER:
        if u > 0:
            loads[u].start()
    load_lk.start()
    load_lv.start()
    for c in small:
        c.start()

    mine = pl.ds(pl.multiple_of(f * 512, 512), 512)
    theirs = pl.ds(pl.multiple_of((1 - f) * 512, 512), 512)

    def own_half(u, place):
        def memory_rows(c, _):
            at = pl.ds(pl.multiple_of(c * 256, 256), 256)
            place[at, :] = dot(memory[at, mine], own[u])
            return 0

        lax.fori_loop(0, 4, memory_rows, 0)

    pl.semaphore_wait(barrier, 16 + 4 + 1 + 3 + 1 + 2 + 1)

    def first_copy(j):
        t = 2 * lax.rem(j + lax.div(over, 2), 16) + (1 - m)
        return remote(
            feat.at[:, :, pl.ds(pl.multiple_of(t * 128, 128), 128)],
            gath.at[lax.div(k, 2)],
            sent.at[0],
            g_recv.at[0],
            dev(lax.rem(2 * t + 32, 64) + odd, f, lax.rem(k, 2)),
        )

    def send_first(j, _):
        first_copy(j).start()
        return 0

    load_feat.wait()
    lax.fori_loop(0, 16, send_first, 0)

    def part_of(ref, u, at, count=64):
        return ref.at[u, pl.ds(pl.multiple_of(at, 32), count), :]

    def direct(c, parity):
        return lax.rem(c + 8, 4) * 128 + parity * 64

    def around(step):
        return lax.rem(z + 8 + step, 8) * 64

    zp = lax.rem(z, 2)

    def mine_of(u, c):
        if KIND[u] == 0:
            return part_of(got, u, direct(c, 0), 128)
        return part_of(got, u, direct(c, zp) if KIND[u] == 1 else around(0))

    def cross_copy(u):
        if KIND[u] == 0:
            at, count = direct(color + 2, 0), 128
        else:
            at, count = direct(color + 2, zp) if KIND[u] == 1 else around(0), 64
        return remote(
            part_of(own, u, at, count),
            part_of(got, u, at, count),
            sent.at[3 + u],
            c_recv.at[u],
            cross_dev,
        )

    def swap_copy(u):
        ref = part_of(got, u, direct(color, zp))
        return remote(ref, ref, sent.at[3 + u], s_recv.at[KIND[:u].count(1)], z_pair)

    def forward_copy(u, i, late):
        ref = part_of(got, u, direct(color, 1 - zp)) if late else mine_of(u, color)
        return remote(ref, ref, sent.at[3 + u], f_recv.at[u], ring[i])

    def ring_place(u, hop, way, half):
        at = around(hop * (2 * way - 1))
        return part_of(got, u, at + 32 * way, 32) if half else part_of(got, u, at)

    def ring_copy(u, step, way):
        ref = ring_place(u, step, way, step == 3)
        return remote(ref, ref, sent.at[3 + u], z_recv.at[KIND[:u].count(2), step], (z_up, z_down)[way])

    def arrived(ref, sem):
        pltpu.make_async_copy(ref, ref, sem).wait()

    def forward(u):
        arrived(mine_of(u, color), c_recv.at[u])
        if KIND[u] == 1:
            swap_copy(u).start()
        for i in range(3):
            forward_copy(u, i, False).start()

    def second(u):
        arrived(part_of(got, u, direct(color, 1 - zp)), s_recv.at[KIND[:u].count(1)])
        for i in range(3):
            forward_copy(u, i, True).start()

    def ring_arrived(u, step):
        arrived(part_of(got, u, 0, 64 if step == 3 else 128), z_recv.at[KIND[:u].count(2), step])

    def circulate(u, step):
        if step > 0:
            ring_arrived(u, step - 1)
        else:
            arrived(mine_of(u, color), c_recv.at[u])
        for way in range(2):
            ring_copy(u, step, way).start()

    def ready(u):
        if KIND[u] == 2:
            ring_arrived(u, 3)
        else:
            arrived(part_of(got, u, 0, 384), f_recv.at[u])

    def across(units):
        for u in units:
            if u > 0 or u in ORDER[:EARLY]:
                loads[u].wait()
            cross_copy(u).start()

    across(ORDER[:EARLY])

    def build_perm(s, _):
        at = lax.broadcasted_iota(jnp.int32, (128, 1024), 0)
        col = lax.broadcasted_iota(jnp.int32, (128, 1024), 1)
        want = (at >> 3) * 64 + lax.div(s, 4) * 32 + lax.rem(s, 4) * 8 + (at & 7)
        perm[pl.ds(pl.multiple_of(s * 128, 128), 128), :] = jnp.where(
            col == want, 1.0, 0.0
        ).astype(BF16)
        return 0

    lax.fori_loop(0, 8, build_perm, 0)
    at = lax.broadcasted_iota(jnp.int32, (STR * ROWS, STR * FRAMES), 0)
    col = lax.broadcasted_iota(jnp.int32, (STR * ROWS, STR * FRAMES), 1)
    rows[...] = jnp.where(col == (at & 7) * STR + (at >> 3), 1.0, 0.0).astype(BF16)
    at = lax.broadcasted_iota(jnp.int32, (STR * FRAMES, STR * ROWS), 0)
    col = lax.broadcasted_iota(jnp.int32, (STR * FRAMES, STR * ROWS), 1)
    frames_first[...] = jnp.where(col == (at & 31) * ROWS + (at >> 5), 1.0, 0.0).astype(BF16)
    att[...] = jnp.zeros_like(att)

    load_mem.wait()
    if 0 not in ORDER[:EARLY]:
        loads[0].wait()
    own_half(0, k_half)

    def second_copy(e):
        rr, to = quad(e)
        return remote(blocks.at[rr], held.at[m, r], sent.at[1], h_recv.at[0], to)

    def relay_copy():
        return remote(held.at[m], held.at[m], sent.at[2], h_recv.at[1], sibling)

    def relay():
        arrived(held.at[m], h_recv.at[0])
        relay_copy().start()

    def send_second(e, _):
        second_copy(e).start()
        return 0

    def turn():
        arrived(gath, g_recv.at[0])
        for fr in range(FRAMES):
            turned = gath[:, fr].astype(F32).reshape(128, 128).T.astype(BF16)
            blocks[:, fr] = turned.reshape(4, STR, 128)
        lax.fori_loop(0, 4, send_second, 0)
        across(ORDER[EARLY:])

    def split_norm(values_f32, chunk):
        at = pl.ds(pl.multiple_of(chunk * 32, 32), 32)
        b = values_f32.astype(BF16)
        n[0, at, :] = b[:, :512]
        n[1, at, :] = b[:, 512:]

    def first_norm(c, _):
        at = pl.ds(pl.multiple_of(c * 32, 32), 32)
        v = normalized(x[at, :]).astype(BF16).astype(F32).reshape(4, ROWS, 1024)
        row = lax.broadcasted_iota(jnp.int32, v.shape, 1)
        summary = jnp.sum(jnp.where(row < GROUP, v, 0.0), axis=1, keepdims=True) * (1.0 / GROUP)
        v = jnp.where(row == FRAMES, summary, v)
        split_norm(v.reshape(32, 1024), c)
        return 0

    def norm():
        arrived(held.at[1 - m], h_recv.at[1])
        for s in range(8):
            xp[:, pl.ds(128 * s, 128)] = held[s // 4, s % 4].reshape(STR * FRAMES, 128)
        for h in range(2):
            half = pl.ds(512 * h, 512)
            placed = dot(xp[...], perm[:, half]).astype(BF16)
            x[:, half] = dot(rows[...], placed)
        lax.fori_loop(0, 8, first_norm, 0, unroll=4)

    ready_once = set()

    def need(u):
        if u not in ready_once:
            ready_once.add(u)
            ready(u)

    def other_half(u, half, place):
        need(u)

        def memory_rows(c, _):
            at = pl.ds(pl.multiple_of(c * 256, 256), 256)
            sums = half[at, :] + dot(memory[at, theirs], got[u])
            place[pl.ds(c * 8, 8), pl.ds(0, MEM), :] = sums.astype(BF16).reshape(8, MEM, 512)
            return 0

        lax.fori_loop(0, 4, memory_rows, 0)

    def group(u, place, center):
        need(u)

        g = (dot(n[f], own[u]) + dot(n[1 - f], got[u])).reshape(STR, ROWS, 512)
        both = jnp.concatenate([g, jnp.zeros_like(g)], axis=1).astype(BF16)
        place[:, pl.ds(MEM + LEFT, 16), :] = both
        center[...] = g[:, :GROUP, :].astype(BF16)

    def query():
        need(2)
        q[...] = (
            (dot(n[f], own[2]) + dot(n[1 - f], got[2])).astype(BF16).astype(F32) * (HD**-0.5)
        ).reshape(STR, ROWS, 512)

    heads = ROWS
    head_mask = jnp.where(
        (lax.broadcasted_iota(jnp.int32, (heads, 512), 1) >> 6)
        == lax.broadcasted_iota(jnp.int32, (heads, 512), 0),
        1.0,
        0.0,
    )
    queries = FRAMES + 1

    width = 8

    def attend(first):
        streams = [first + i for i in range(width)]
        probs = []
        scored = []
        for s in streams:
            q8 = q[s]
            spread = jnp.concatenate(
                [
                    jnp.broadcast_to(q8[i : i + 1], (heads, 512)) * head_mask
                    for i in range(queries)
                ],
                axis=0,
            ).astype(BF16)
            scored.append(
                lax.dot_general(
                    spread, keys[s], (((1,), (1,)), ((), ())), preferred_element_type=F32
                )
            )
        row = lax.broadcasted_iota(jnp.int32, (queries * heads, KEYS), 0)
        col = lax.broadcasted_iota(jnp.int32, (queries * heads, KEYS), 1)
        in_mem = (col < MEM) & (row < FRAMES * heads)
        in_rest = col < MEM + LEFT + FRAMES
        for s, scores in zip(streams, scored):
            seen_mem = (col >= MEM - fill[s]) & in_mem
            seen_left = (col >= MEM + LEFT - length[s]) & in_rest
            scores = jnp.where(seen_mem | seen_left, scores, MASKED)
            e = jnp.exp(scores - jnp.max(scores, axis=-1, keepdims=True))
            probs.append((e / jnp.sum(e, axis=-1, keepdims=True)).astype(BF16))
        for s, p in zip(streams, probs):
            mixed = dot(p, values[s]).reshape(queries, heads, 512)
            att[s, pl.ds(0, queries), :] = jnp.sum(mixed * head_mask[None], axis=1)

    def attend_block(b):
        def few(i, _):
            attend(b * 8 + width * i)
            return 0

        lax.fori_loop(0, 8 // width, few, 0)

    def exchange(src, dst, i):
        return remote(src, dst, e_send.at[i], e_recv.at[i], sibling)

    def output():
        need(3)
        a = att[...].reshape(STR * ROWS, 512).astype(BF16)
        for i, (h, w) in enumerate(((f, own), (1 - f, got))):
            part[h] = dot(a, w[3]).astype(BF16)
            exchange(part.at[h], part_in.at[h], i).start()

    def second_norm(c, _):
        at = pl.ds(pl.multiple_of(c * 32, 32), 32)
        summed = [part[h, at, :].astype(F32) + part_in[h, at, :].astype(F32) for h in range(2)]
        v = x[at, :] + jnp.concatenate(summed, axis=1)
        x[at, :] = v
        split_norm(normalized(v), c)
        return 0

    def norm_two():
        for i, h in enumerate((f, 1 - f)):
            exchange(part.at[h], part_in.at[h], i).wait()
        lax.fori_loop(0, 8, second_norm, 0, unroll=4)

    def next_memory():
        mem_vm[...] = jnp.tanh(x[...].reshape(STR, ROWS, 1024)[:, FRAMES, :]).astype(BF16)
        write[1].start()

    hidden = {}

    def hidden_block(j):
        need(4 + 2 * j)
        sums = dot(n[f], own[4 + 2 * j]) + dot(n[1 - f], got[4 + 2 * j])
        hidden[j] = jax.nn.gelu(sums, approximate=True).astype(BF16)

    def down_block(j):
        need(5 + 2 * j)
        for i, (h, w) in enumerate(((f, own), (1 - f, got))):
            sums = dot(hidden[j], w[5 + 2 * j])
            if j != BLOCKS[0]:
                sums = down[h] + sums
            if j != BLOCKS[3]:
                down[h] = sums
                continue
            down_out[h] = sums.astype(BF16)
            exchange(down_out.at[h], down_in.at[h], 2 + i).start()

    def third_norm(c, _):
        at = pl.ds(pl.multiple_of(c * 32, 32), 32)
        summed = [down_out[h, at, :].astype(F32) + down_in[h, at, :].astype(F32) for h in range(2)]
        v = x[at, :] + jnp.concatenate(summed, axis=1)
        split_norm(normalized(v) * gain[...], c)
        return 0

    def finish():
        for i, h in enumerate((f, 1 - f)):
            exchange(down_out.at[h], down_in.at[h], 2 + i).wait()
        lax.fori_loop(0, 8, third_norm, 0, unroll=4)
        for h in range(2):
            placed = dot(frames_first[...], n[h]).astype(BF16)
            out_vm[:, :, pl.ds(512 * h, 512)] = placed.reshape(FRAMES, STR, 512)
        write[0].start()

    def keys_done():
        for c in small:
            c.wait()
        load_lk.wait()
        other_half(0, k_half, keys)

    def values_done():
        load_lv.wait()
        other_half(1, v_half, values)

    def group_k():
        group(0, keys, ck_vm)
        write[2].start()

    def group_v():
        group(1, values, cv_vm)
        write[3].start()

    steps = {
        "own_v": lambda: own_half(1, v_half),
        "turn": turn,
        "norm": norm,
        "relay": relay,
        "mem_k": keys_done,
        "mem_v": values_done,
        "group_k": group_k,
        "group_v": group_v,
        "query": query,
        "output": output,
        "norm_two": norm_two,
        "next": next_memory,
        "finish": finish,
    }
    more = {
        "forward": forward,
        "second": second,
        "circulate": circulate,
        "attend": attend_block,
        "hidden": hidden_block,
        "down": down_block,
    }
    for name, *given in STEPS:
        if name in steps:
            steps[name]()
        else:
            more[name](*given)

    arrived(gath, sent.at[0])
    arrived(held.at[m], sent.at[1])
    arrived(held.at[m], sent.at[2])
    for u in range(UNITS):
        arrived(got.at[u], sent.at[3 + u])
    for copy in write:
        copy.wait()


def hand_over(*refs):
    sems = refs[8]
    leave = [pltpu.make_async_copy(refs[i], refs[4 + i], sems.at[i]) for i in range(4)]
    for copy in leave:
        copy.start()
    for copy in leave:
        copy.wait()


def shards(
    features,
    memory_bank,
    memory_fill,
    left_keys,
    left_values,
    left_length,
    w_query,
    w_key,
    w_value,
    w_out,
    w_up,
    w_down,
    out_gain,
):
    memory = memory_bank.reshape(STR * MEM, 1024)
    hbm = pl.BlockSpec(memory_space=pltpu.HBM)
    either = pl.BlockSpec(memory_space=pl.ANY)
    dma = pltpu.SemaphoreType.DMA
    shapes = (
        jax.ShapeDtypeStruct((FRAMES, STR, 1024), BF16),
        jax.ShapeDtypeStruct((STR, 1024), BF16),
        jax.ShapeDtypeStruct((STR, GROUP, 512), BF16),
        jax.ShapeDtypeStruct((STR, GROUP, 512), BF16),
    )
    results = pl.pallas_call(
        kernel,
        name="layer",
        out_shape=shapes,
        in_specs=[hbm] * 13,
        out_specs=(either,) * 4,
        scratch_shapes=[
            pltpu.VMEM((FRAMES, 8, 4096), BF16),
            pltpu.VMEM((16, FRAMES, 8, 128), BF16),
            pltpu.VMEM((4, FRAMES, STR, 128), BF16),
            pltpu.VMEM((2, 4, FRAMES, STR, 128), BF16),
            pltpu.VMEM((1024, 1024), BF16),
            pltpu.VMEM((STR * ROWS, STR * FRAMES), BF16),
            pltpu.VMEM((STR * FRAMES, STR * ROWS), BF16),
            pltpu.VMEM((STR * FRAMES, 1024), BF16),
            pltpu.VMEM((STR * ROWS, 1024), F32),
            pltpu.VMEM((2, STR * ROWS, 512), BF16),
            pltpu.VMEM((UNITS, 512, 512), BF16),
            pltpu.VMEM((UNITS, 512, 512), BF16),
            pltpu.VMEM((STR * MEM, 1024), BF16),
            pltpu.VMEM((STR, KEYS, 512), BF16),
            pltpu.VMEM((STR, KEYS, 512), BF16),
            pltpu.VMEM((STR, ROWS, 512), F32),
            pltpu.VMEM((STR, ROWS, 512), F32),
            pltpu.VMEM((2, STR * ROWS, 512), BF16),
            pltpu.VMEM((2, STR * ROWS, 512), BF16),
            pltpu.VMEM((2, STR * ROWS, 512), F32),
            pltpu.VMEM((2, STR * ROWS, 512), BF16),
            pltpu.VMEM((2, STR * ROWS, 512), BF16),
            pltpu.VMEM((STR * MEM, 512), F32),
            pltpu.VMEM((STR * MEM, 512), F32),
            *[pltpu.VMEM(v.shape, v.dtype) for v in shapes],
            pltpu.SMEM((STR,), jnp.int32),
            pltpu.SMEM((STR,), jnp.int32),
            pltpu.VMEM((1, 1024), F32),
            dma((4,)),
            dma((UNITS + 7,)),
            dma((3 + UNITS,)),
            dma((1,)),
            dma((2,)),
            dma((UNITS,)),
            dma((max(1, KIND.count(1)),)),
            dma((UNITS,)),
            dma((max(1, KIND.count(2)), 4)),
            dma((4,)),
            dma((4,)),
        ],
        compiler_params=pltpu.CompilerParams(
            collective_id=0, has_side_effects=True, vmem_limit_bytes=46_000_000
        ),
    )(
        *[
            pltpu.with_memory_space_constraint(v, pltpu.HBM)
            for v in (
                memory_fill,
                left_length,
                features,
                memory,
                left_keys,
                left_values,
                w_query,
                w_key,
                w_value,
                w_out,
                w_up,
                w_down,
                out_gain.reshape(1, 1024),
            )
        ]
    )
    layer_out, memory_next, center_keys, center_values = pl.pallas_call(
        hand_over,
        name="hand_over",
        out_shape=shapes,
        in_specs=[either] * 4,
        out_specs=(hbm,) * 4,
        scratch_shapes=[dma((4,))],
        compiler_params=pltpu.CompilerParams(vmem_limit_bytes=1_000_000),
    )(*results)
    return jnp.transpose(layer_out, (1, 0, 2)), memory_next, center_keys, center_values


def solution(mesh):
    in_specs = (
        P(None, ("dp", "fsdp"), None),
        P(("dp", "fsdp"), None, None),
        P(("dp", "fsdp")),
        P(("dp", "fsdp"), None, "mp"),
        P(("dp", "fsdp"), None, "mp"),
        P(("dp", "fsdp")),
        P("fsdp", "mp"),
        P("fsdp", "mp"),
        P("fsdp", "mp"),
        P("mp", "fsdp"),
        P("fsdp", "mp"),
        P("mp", "fsdp"),
        P(),
    )
    out_specs = (
        P(("dp", "fsdp"), None, None),
        P(("dp", "fsdp"), None),
        P(("dp", "fsdp"), None, "mp"),
        P(("dp", "fsdp"), None, "mp"),
    )
    return jax.shard_map(shards, mesh=mesh, in_specs=in_specs, out_specs=out_specs, check_vma=False)
```
